256 devices in a mesh: groups: 4 (over y, x), row: 32 (over z), col: 2 (over core).
Axes of the slice: x: 2, y: 2, z: 32, core: 2. Of those that a mesh axis runs over, the one named last changes fastest.
The devices are a block of a 4x8x32 slice.
Arguments:
- pair_rep: bfloat16 [1024, 256, 128], P(('groups', 'row'), 'col'), parts along dimension 0, may hold values from -6 to 6
- residue_mask: int32 [1024], P('groups'), parts along dimension 0, may hold values 0 or 1
- crop_length: int32 [4], P('groups'), parts along dimension 0, may hold values from 128 to 256
- norm_gain: float32 [2, 128], replicated, may hold values from 0.25 to 1.75
- mult_proj: bfloat16 [2, 128, 640], replicated, may hold values from -0.5 to 0.5
- mixed_gain: float32 [2, 128], replicated, may hold values from 0.25 to 1.75
- mult_out: bfloat16 [2, 128, 128], replicated, may hold values from -0.5 to 0.5
- att_gain: float32 [128], replicated, may hold values from 0.25 to 1.75
- att_proj: bfloat16 [128, 512], replicated, may hold values from -5 to 5
- att_bias: bfloat16 [128, 4], replicated, may hold values from -0.5 to 0.5
- att_out: bfloat16 [128, 128], replicated, may hold values from -0.5 to 0.5
Outputs:
- pair_out: bfloat16 [1024, 256, 128], P(('groups', 'row'), 'col'), parts along dimension 0
The draws below stay inside these ranges and needn't reach their ends.
There are 4 independent parts, one for each index of `groups`. The reference program is written for one: setup_inputs(seed, part) draws one part's arguments, and reference() takes and returns one part's arrays. A program takes and returns all parts, laid end to end along the dimension named above; an argument that names none is the same for every part. Nothing has to cross between parts.
All inputs are finite; a program needn't handle non-finite values.
Results may differ from the reference program's by a relative error of at most 0.03.
Values may be sent and summed in bfloat16 or wider, within the bound.
A program may use at most 64 MiB of HBM per device.

```python
import jax
import jax.numpy as jnp
from jax import lax

C = 128
HID = 128
HEADS = 4
HEAD_DIM = 32
ATT = 128
NRES = 256


def draw_att_proj(key, part):
    drawn = jax.random.normal(key, (C, 4 * ATT), jnp.float32) * C ** (-0.5)
    return jnp.clip(drawn, -5.0, 5.0).astype(jnp.bfloat16)


def touch_ends(values, stream_key, smallest, top_value):
    longest = values.shape.index(max(values.shape))
    spots = []
    for shift in (0, 1):
        where = [jax.random.randint(jax.random.fold_in(stream_key, axis), (), 0, length) for axis, length in enumerate(values.shape)]
        where[longest] = (where[longest] + shift) % values.shape[longest]
        spots.append(tuple(where))
    return values.at[spots[0]].set(smallest).at[spots[1]].set(top_value)


def block_scale(own_key, dims, pieces, smallest, top_value):
    def one(position, shards_of):
        heights = jax.random.uniform(jax.random.fold_in(jax.random.fold_in(own_key, 6), position), (shards_of,), jnp.float32, smallest / len(pieces), top_value / len(pieces))
        return jnp.repeat(jnp.exp(heights), dims[position] // shards_of).reshape((-1,) + (1,) * (len(dims) - position - 1))

    level = one(*pieces[0])
    for cut in pieces[1:]:
        level = level * one(*cut)
    return level


def centred(own_key, dims, deviation, reach, split=(), kind=jnp.bfloat16):
    entries = deviation * jax.random.normal(own_key, dims, jnp.float32)
    if split:
        entries = entries * block_scale(own_key, dims, split, -0.22, 0.18)
    return jnp.clip(entries, -reach, reach).astype(kind)


def setup_inputs(seed: int = 0, part: int = 0) -> dict:
    arg_keys = jax.random.split(jax.random.key(seed), 12)
    part_splits = jax.random.split(jax.random.fold_in(arg_keys[11], part), 12)
    pair_rep = centred(part_splits[0], (NRES, NRES, C), 1.0, 6.0, ((0, 32), (1, 2)))
    residue_mask = touch_ends((jax.random.randint(part_splits[1], (NRES,), 0, 8) < 7).astype(jnp.int32), jax.random.fold_in(part_splits[1], 1), 0, 1)
    crop_length = jax.random.randint(part_splits[2], (1,), NRES // 2, NRES + 1).astype(jnp.int32)
    norm_gain = jnp.clip(1.0 + 0.15 * jax.random.normal(arg_keys[3], (2, C), jnp.float32), 0.25, 1.75)
    mult_proj = centred(arg_keys[4], (2, C, 4 * HID + C), C ** -0.5, 0.5)
    mixed_gain = jnp.clip(1.0 + 0.15 * jax.random.normal(arg_keys[5], (2, HID), jnp.float32), 0.25, 1.75)
    mult_out = centred(arg_keys[6], (2, HID, C), HID ** -0.5, 0.5)
    att_gain = jnp.clip(1.0 + 0.15 * jax.random.normal(arg_keys[7], (C,), jnp.float32), 0.25, 1.75)
    att_proj = draw_att_proj(jax.random.fold_in(arg_keys[11], 71), part)
    att_bias = centred(arg_keys[9], (C, HEADS), C ** -0.5, 0.5)
    att_out = centred(arg_keys[10], (ATT, C), ATT ** -0.5, 0.5)
    return dict(pair_rep=pair_rep, residue_mask=residue_mask, crop_length=crop_length, norm_gain=norm_gain, mult_proj=mult_proj, mixed_gain=mixed_gain, mult_out=mult_out, att_gain=att_gain, att_proj=att_proj, att_bias=att_bias, att_out=att_out)


EPSILON = 1e-05

def normalize(values, gain_vec, along):
    average = lax.optimization_barrier(jnp.mean(values, axis=along, keepdims=True))
    centered = values - average
    variance = lax.optimization_barrier(jnp.mean(centered * centered, axis=along, keepdims=True))
    return centered * lax.rsqrt(variance + EPSILON) * gain_vec

def live_mask(residue_mask, crop_length):
    positions = jnp.arange(residue_mask.shape[0], dtype=jnp.int32)
    alive = ((residue_mask == 1) | (positions == 0)) & (positions < crop_length[0])
    return alive.astype(jnp.float32)

def triangle_update(pair_rep, gain_vec, proj_w, out_gain, out_w, pair_mask, incoming):
    normed = normalize(pair_rep.astype(jnp.float32), gain_vec, -1).astype(jnp.bfloat16)
    projected = jnp.dot(normed.reshape(-1, C), proj_w, preferred_element_type=jnp.float32)
    projected = projected.reshape(NRES, NRES, 4 * HID + C)
    masked = pair_mask[:, :, None]
    left_proj = (masked * jax.nn.sigmoid(projected[..., HID:2 * HID]) * projected[..., :HID]).astype(jnp.bfloat16)
    right_proj = (masked * jax.nn.sigmoid(projected[..., 3 * HID:4 * HID]) * projected[..., 2 * HID:3 * HID]).astype(jnp.bfloat16)
    gate_lin = projected[..., 4 * HID:]
    if incoming:
        product = jnp.einsum('kic,kjc->ijc', left_proj.astype(jnp.float32), right_proj.astype(jnp.float32))
    else:
        product = jnp.einsum('ikc,jkc->ijc', left_proj.astype(jnp.float32), right_proj.astype(jnp.float32))
    mixed = product.astype(jnp.bfloat16)
    mixed_norm = normalize(mixed.astype(jnp.float32), out_gain, -1).astype(jnp.bfloat16)
    update = jnp.dot(mixed_norm.reshape(-1, HID), out_w, preferred_element_type=jnp.float32).reshape(NRES, NRES, C)
    return (pair_rep.astype(jnp.float32) + jax.nn.sigmoid(gate_lin) * update).astype(jnp.bfloat16)

def reference(pair_rep, residue_mask, crop_length, norm_gain, mult_proj, mixed_gain, mult_out, att_gain, att_proj, att_bias, att_out):
    alive = live_mask(residue_mask, crop_length)
    pair_mask = alive[:, None] * alive[None, :]
    first = triangle_update(pair_rep, norm_gain[0], mult_proj[0], mixed_gain[0], mult_out[0], pair_mask, False)
    second = triangle_update(first, norm_gain[1], mult_proj[1], mixed_gain[1], mult_out[1], pair_mask, True)
    normed = normalize(second.astype(jnp.float32), att_gain, -1).astype(jnp.bfloat16)
    projected = jnp.dot(normed.reshape(-1, C), att_proj, preferred_element_type=jnp.float32).reshape(NRES, NRES, 4 * ATT)
    queries = projected[..., :ATT].astype(jnp.bfloat16)
    key_rows = projected[..., ATT:2 * ATT].astype(jnp.bfloat16)
    value_rows = projected[..., 2 * ATT:3 * ATT].astype(jnp.bfloat16)
    gates = projected[..., 3 * ATT:].astype(jnp.bfloat16)
    tri_bias = jnp.dot(normed.reshape(-1, C), att_bias, preferred_element_type=jnp.float32)
    tri_bias = tri_bias.astype(jnp.bfloat16).reshape(NRES, NRES, HEADS)
    bias_heads = jnp.transpose(tri_bias.astype(jnp.float32), (2, 0, 1))
    key_mask = jnp.where(alive > 0, 0.0, -1000000000.0).astype(jnp.float32)
    scaling = 1.0 / math_sqrt(HEAD_DIM)

    def one_row(items):
        query_row, key_row, value_row, gate_row = items
        query_row = query_row.reshape(NRES, HEADS, HEAD_DIM).astype(jnp.float32)
        key_row = key_row.reshape(NRES, HEADS, HEAD_DIM).astype(jnp.float32)
        value_row = value_row.reshape(NRES, HEADS, HEAD_DIM).astype(jnp.float32)
        scores = jnp.einsum('jhd,khd->hjk', query_row, key_row) * scaling + bias_heads + key_mask[None, None, :]
        weights = jax.nn.softmax(scores, axis=-1).astype(jnp.bfloat16)
        attended = jnp.einsum('hjk,khd->jhd', weights.astype(jnp.float32), value_row).reshape(NRES, ATT)
        return (jax.nn.sigmoid(gate_row.astype(jnp.float32)) * attended).astype(jnp.bfloat16)
    gated = lax.map(one_row, (queries, key_rows, value_rows, gates))
    result = jnp.dot(gated.reshape(-1, ATT), att_out, preferred_element_type=jnp.float32).reshape(NRES, NRES, C)
    return (second.astype(jnp.float32) + result).astype(jnp.bfloat16)

def math_sqrt(number):
    return float(number) ** 0.5
```

```python
import functools

import jax
import jax.numpy as jnp
from jax import lax
from jax.experimental import pallas as pl
from jax.experimental.pallas import tpu as pltpu
from jax.sharding import PartitionSpec as P

HEADS = 4
EPSILON = 1e-05
MESH = pl.DeviceIdType.MESH
F32 = jnp.float32
BF16 = jnp.bfloat16
NN = (((1,), (0,)), ((), ()))
NT = (((1,), (1,)), ((), ()))
TN = (((0,), (0,)), ((), ()))


def dot(a, b, dims):
    return lax.dot_general(a, b, dims, preferred_element_type=F32)


def norm_lanes(v, gain):
    mean = jnp.mean(v, axis=-1, keepdims=True)
    cen = v - mean
    var = jnp.mean(cen * cen, axis=-1, keepdims=True)
    return cen * lax.rsqrt(var + EPSILON) * gain


def norm_sublanes(v, gain):
    mean = jnp.mean(v, axis=0, keepdims=True)
    cen = v - mean
    var = jnp.mean(cen * cen, axis=0, keepdims=True)
    return cen * lax.rsqrt(var + EPSILON) * gain


def kernel(
    nz, nc, rows, x_ref, pm_ref, km_ref, ng_ref, mp_ref, mg_ref, mo_ref, ag_ref, ap_ref, ab_ref, ao_ref,
    out_ref,
    wt, mgt, apt, abt, nrm, gate, zb, fl, fr, s_lr, r_lr, s_p, r_p, nall, fb, s_b, r_b, bt, sc, vt, sg,
    sem_lr_s, sem_lr_r, sem_p_s, sem_p_r, sem_n, sem_b,
):
    z = lax.axis_index("row")
    c = lax.axis_index("col")
    me = z * nc + c
    devs = nz * nc
    cols = pm_ref.shape[1]
    ch = x_ref.shape[1]
    per = s_lr.shape[0]
    block = devs * rows
    half = nz // 2
    other = 1 - c

    barrier = pltpu.get_barrier_semaphore()

    def greet(t, carry):
        zz = lax.rem(z + t, nz)
        for cc in range(nc):
            pl.semaphore_signal(barrier, inc=1, device_id={"row": zz, "col": cc}, device_id_type=MESH)
        return carry

    pl.semaphore_signal(barrier, inc=1, device_id={"row": z, "col": other}, device_id_type=MESH)
    lax.fori_loop(1, nz, greet, 0)

    def remote(src, dst, ssem, rsem, zz, cc):
        return pltpu.make_async_remote_copy(
            src_ref=src, dst_ref=dst, send_sem=ssem, recv_sem=rsem,
            device_id={"row": zz, "col": cc}, device_id_type=MESH,
        )

    def far_first(step):
        d = half - (step + 1) // 2
        off = jnp.where(lax.rem(step, 2) == 1, d, nz - d)
        return lax.rem(z + off, nz)

    def scatter(src_at, dst, ssem, rsem):
        def one(step, carry):
            zz = far_first(step)
            for cc in range(nc):
                to = lax.rem(c + cc, nc)
                remote(src_at(zz, to), dst, ssem, rsem, zz, to).start()
            return carry

        lax.fori_loop(0, nz - 1, one, 0)
        remote(src_at(z, other), dst, ssem, rsem, z, other).start()

    def landed(buf, ssem, rsem):
        every = buf.at[pl.ds(0, devs - 1)]
        return remote(every, every, ssem, rsem, z, other)

    for u in range(2):
        for q in range(4):
            wt[u, q * ch:(q + 1) * ch, :] = jnp.transpose(
                mp_ref[u, :, q * ch:(q + 1) * ch].astype(F32)).astype(BF16)
        mgt[u] = jnp.transpose(jnp.broadcast_to(mg_ref[u:u + 1, :], (ch, ch)))

    def project(u, r):
        sl = pl.ds(pl.multiple_of(r * cols, cols), cols)
        src = x_ref if u == 0 else zb
        normed = norm_lanes(src[sl, :].astype(F32), ng_ref[u:u + 1, :]).astype(BF16)
        nrm[sl, :] = normed
        pt = dot(wt[u], normed, NT)
        mask = pm_ref[pl.ds(r, 1), :]
        left = mask * jax.nn.sigmoid(pt[ch:2 * ch]) * pt[:ch]
        right = mask * jax.nn.sigmoid(pt[3 * ch:]) * pt[2 * ch:3 * ch]
        fl[pl.ds(r, ch, stride=rows), :] = left
        fr[pl.ds(r, ch, stride=rows), :] = right

    def send_lr(u, k):
        pair = jnp.concatenate(
            [
                fl[k * block:(k + 1) * block, :].reshape(devs, rows, cols),
                fr[k * block:(k + 1) * block, :].reshape(devs, rows, cols),
            ],
            axis=1,
        )
        s_lr[k] = pair.astype(BF16)
        r_lr[u, k, c * nz + z] = s_lr[k, me]
        scatter(
            lambda zz, cc: s_lr.at[k, zz * nc + cc], r_lr.at[u, k, c * nz + z],
            sem_lr_s.at[k], sem_lr_r.at[u, k])

    def gate_row(u):
        def one(r, carry):
            sl = pl.ds(pl.multiple_of(r * cols, cols), cols)
            gate[sl, :] = jax.nn.sigmoid(dot(nrm[sl, :], mp_ref[u, :, 4 * ch:], NN))
            return carry

        lax.fori_loop(0, rows, one, 0)

    def product(u, k):
        wait = landed(r_lr.at[u, k], sem_lr_s.at[k], sem_lr_r.at[u, k])
        wait.wait_recv()
        lefts, rights = [], []
        for cc in range(nc):
            part = r_lr[u, k, cc * nz:(cc + 1) * nz].astype(F32)
            lefts.append(part[:, :rows].reshape(nz * rows, cols).astype(BF16))
            rights.append(part[:, rows:].reshape(nz * rows, cols).astype(BF16))
        left = jnp.concatenate(lefts, axis=1)
        right = jnp.concatenate(rights, axis=1)
        prod = dot(left, right, NT if u == 0 else TN)
        for cc in range(nc):
            s_p[k, cc] = prod[:, cc * cols:(cc + 1) * cols].reshape(nz, rows, cols).astype(BF16)
        r_p[u, k, me] = s_p[k, c, z]
        scatter(lambda zz, cc: s_p.at[k, cc, zz], r_p.at[u, k, me], sem_p_s.at[k], sem_p_r.at[u, k])
        wait.wait_send()

    def updated(u, r):
        sl = pl.ds(pl.multiple_of(r * cols, cols), cols)
        mixed = norm_sublanes(fl[pl.ds(r, ch, stride=rows), :], mgt[u]).astype(BF16)
        upd = dot(mixed, mo_ref[u], TN)
        src = x_ref if u == 0 else zb
        zb[sl, :] = (src[sl, :].astype(F32) + gate[sl, :] * upd).astype(BF16)

    def rows_loop(f):
        def one(r, carry):
            f(r)
            return carry

        lax.fori_loop(0, rows, one, 0)

    for u in range(2):
        rows_loop(functools.partial(project, u))
        if u == 0:
            pl.semaphore_wait(barrier, devs - 1)
        for k in range(per):
            send_lr(u, k)
        gate_row(u)
        if u == 0:
            for q in range(4):
                apt[q * ch:(q + 1) * ch, :] = jnp.transpose(
                    ap_ref[:, q * ch:(q + 1) * ch].astype(F32)).astype(BF16)
            abt[...] = jnp.transpose(ab_ref[...].astype(F32)).astype(BF16)
        for k in range(per):
            product(u, k)
        for k in range(per):
            wait = landed(r_p.at[u, k], sem_p_s.at[k], sem_p_r.at[u, k])
            wait.wait_recv()
            fl[k * block:(k + 1) * block, :] = r_p[u, k].astype(F32).reshape(block, cols)
            wait.wait_send()
        rows_loop(functools.partial(updated, u))

    def normed_row(r):
        sl = pl.ds(pl.multiple_of(r * cols, cols), cols)
        normed = norm_lanes(zb[sl, :].astype(F32), ag_ref[...]).astype(BF16)
        nall[c, sl, :] = normed
        fb[pl.ds(r, abt.shape[0], stride=rows), :] = dot(abt[...], normed, NT)

    rows_loop(normed_row)
    hr = HEADS * rows
    s_b[...] = fb[:hr, :].astype(BF16)
    mine = lax.rem(z, half)
    to = z // half

    def spread(step, carry):
        zz = far_first(step)
        remote(s_b, r_b.at[c * half + mine], sem_b.at[0], sem_b.at[1], zz, to).start()
        return carry

    lax.fori_loop(0, nz - 1, spread, 0)

    @pl.when(to == c)
    def _():
        r_b[c * half + mine] = s_b[...]

    @pl.when(to != c)
    def _():
        remote(s_b, r_b.at[c * half + mine], sem_b.at[0], sem_b.at[1], z, other).start()

    swap = remote(nall.at[c], nall.at[c], sem_n.at[0], sem_n.at[1], z, other)
    swap.start()
    swap.wait()

    def scores_row(r):
        sl = pl.ds(pl.multiple_of(r * cols, cols), cols)
        mine_n = nall[c, sl, :]
        full = jnp.concatenate([nall[cc, sl, :] for cc in range(nc)], axis=0)
        qt = dot(apt[:ch], mine_n, NT).astype(BF16)
        gt = dot(apt[3 * ch:], mine_n, NT).astype(BF16)
        keys = dot(full, ap_ref[:, ch:2 * ch], NN).astype(BF16)
        vt[r] = dot(apt[2 * ch:3 * ch], full, NT).astype(BF16)
        sg[r] = jax.nn.sigmoid(gt.astype(F32))
        hd = ch // HEADS
        wide = []
        for h in range(HEADS):
            parts = [jnp.zeros((h * hd, cols), BF16)] if h else []
            parts.append(qt[h * hd:(h + 1) * hd])
            if h < HEADS - 1:
                parts.append(jnp.zeros(((HEADS - 1 - h) * hd, cols), BF16))
            wide.append(jnp.concatenate(parts, axis=0))
        sc[r] = dot(keys, jnp.concatenate(wide, axis=1), NN)

    rows_loop(scores_row)

    def bias_wait(count):
        return remote(r_b.at[pl.ds(0, count)], r_b.at[pl.ds(0, count)], sem_b.at[0], sem_b.at[1], z, other)

    @pl.when(to == c)
    def _():
        bias_wait(nz - 1).wait()

    @pl.when(to != c)
    def _():
        bias_wait(nz).wait()

    for kc in range(nc):
        part = r_b[kc * half:(kc + 1) * half].astype(F32)
        for h in range(HEADS):
            tile = part[:, h * rows:(h + 1) * rows].reshape(half * rows, cols) + km_ref[kc:kc + 1, :]
            bt[kc * cols:(kc + 1) * cols, h * cols:(h + 1) * cols] = jnp.transpose(tile)

    hd = ch // HEADS
    scale = 1.0 / float(hd) ** 0.5

    def attend_row(r):
        sl = pl.ds(pl.multiple_of(r * cols, cols), cols)
        score = sc[r] * scale + bt[...]
        top = jnp.max(score, axis=0, keepdims=True)
        e = jnp.exp(score - top)
        inv = 1.0 / jnp.sum(e, axis=0, keepdims=True)
        got = dot(vt[r], e.astype(BF16), NN)
        parts = []
        for h in range(HEADS):
            lanes = slice(h * cols, (h + 1) * cols)
            parts.append(got[h * hd:(h + 1) * hd, lanes] * inv[:, lanes])
        gated = (sg[r] * jnp.concatenate(parts, axis=0)).astype(BF16)
        out_ref[sl, :] = (zb[sl, :].astype(F32) + dot(gated, ao_ref[...], TN)).astype(BF16)

    rows_loop(attend_row)


def solution(mesh):
    nz, nc = mesh.shape["row"], mesh.shape["col"]
    devs = nz * nc

    def local(pair_rep, residue_mask, crop_length, norm_gain, mult_proj, mixed_gain, mult_out, att_gain, att_proj,
              att_bias, att_out):
        rows, cols, ch = pair_rep.shape
        per = ch // devs
        half = nz // 2
        z, c = lax.axis_index("row"), lax.axis_index("col")
        positions = jnp.arange(residue_mask.shape[0], dtype=jnp.int32)
        alive = (((residue_mask == 1) | (positions == 0)) & (positions < crop_length[0])).astype(F32)
        row_alive = lax.dynamic_slice_in_dim(alive, z * rows, rows, 0)
        col_alive = lax.dynamic_slice_in_dim(alive, c * cols, cols, 0)
        pair_mask = row_alive[:, None] * col_alive[None, :]
        key_mask = jnp.where(alive > 0, 0.0, -1000000000.0).astype(F32).reshape(nc, cols)
        area = rows * cols
        vmem = pltpu.VMEM
        out = pl.pallas_call(
            functools.partial(kernel, nz, nc, rows),
            out_shape=jax.ShapeDtypeStruct((area, ch), BF16),
            in_specs=[pl.BlockSpec(memory_space=vmem)] * 11,
            out_specs=pl.BlockSpec(memory_space=vmem),
            scratch_shapes=[
                vmem((2, 4 * ch, ch), BF16),
                vmem((2, ch, ch), F32),
                vmem((4 * ch, ch), BF16),
                vmem((HEADS, ch), BF16),
                vmem((area, ch), BF16),
                vmem((area, ch), F32),
                vmem((area, ch), BF16),
                vmem((ch * rows, cols), F32),
                vmem((ch * rows, cols), F32),
                vmem((per, devs, 2 * rows, cols), BF16),
                vmem((2, per, devs, 2 * rows, cols), BF16),
                vmem((per, nc, nz, rows, cols), BF16),
                vmem((2, per, devs, rows, cols), BF16),
                vmem((nc, area, ch), BF16),
                vmem((HEADS * rows, cols), F32),
                vmem((HEADS * rows, cols), BF16),
                vmem((nc * half, HEADS * rows, cols), BF16),
                vmem((nc * cols, HEADS * cols), F32),
                vmem((rows, nc * cols, HEADS * cols), F32),
                vmem((rows, ch, nc * cols), BF16),
                vmem((rows, ch, cols), F32),
                pltpu.SemaphoreType.DMA((per,)),
                pltpu.SemaphoreType.DMA((2, per)),
                pltpu.SemaphoreType.DMA((per,)),
                pltpu.SemaphoreType.DMA((2, per)),
                pltpu.SemaphoreType.DMA((2,)),
                pltpu.SemaphoreType.DMA((2,)),
            ],
            compiler_params=pltpu.CompilerParams(
                collective_id=1, has_side_effects=True, vmem_limit_bytes=48 * 1024 * 1024
            ),
            name="triangle",
        )(
            pair_rep.reshape(area, ch), pair_mask, key_mask, norm_gain, mult_proj, mixed_gain, mult_out,
            att_gain.reshape(1, ch), att_proj, att_bias, att_out,
        )
        return out.reshape(rows, cols, ch)

    return jax.shard_map(
        local,
        mesh=mesh,
        in_specs=(P(("groups", "row"), "col", None), P("groups"), P("groups")) + (P(),) * 8,
        out_specs=P(("groups", "row"), "col", None),
        check_vma=False,
    )
```

```python
import functools

import jax
import jax.numpy as jnp
from jax import lax
from jax.experimental import pallas as pl
from jax.experimental.pallas import tpu as pltpu
from jax.sharding import PartitionSpec as P

HEADS = 4
EPSILON = 1e-05
MESH = pl.DeviceIdType.MESH
F32 = jnp.float32
BF16 = jnp.bfloat16
NN = (((1,), (0,)), ((), ()))
NT = (((1,), (1,)), ((), ()))
TN = (((0,), (0,)), ((), ()))


def dot(a, b, dims):
    return lax.dot_general(a, b, dims, preferred_element_type=F32)


def norm_lanes(v, gain):
    mean = jnp.mean(v, axis=-1, keepdims=True)
    cen = v - mean
    var = jnp.mean(cen * cen, axis=-1, keepdims=True)
    return cen * lax.rsqrt(var + EPSILON) * gain


def norm_sublanes(v, gain):
    mean = jnp.mean(v, axis=0, keepdims=True)
    cen = v - mean
    var = jnp.mean(cen * cen, axis=0, keepdims=True)
    return cen * lax.rsqrt(var + EPSILON) * gain


def kernel(
    nz, nc, rows, stride, crop_ref, rm_hbm, x_hbm, ng_hbm, mp_hbm, mg_hbm, mo_hbm, ag_hbm, ap_hbm, ab_hbm, ao_hbm,
    out_ref,
    rm_ref, x_ref, ng_ref, mp_ref, mg_ref, mo_ref, ag_ref, ap_ref, ab_ref, ao_ref, sem_in,
    pm_ref, km_ref, wt, mgt, apt, nrm, gate, zb, fl, fr, s_lr, r_lr, s_p, r_p, nall, fb, s_b, r_b, bt, sc, vt, sg,
    level, sem_lr_s, sem_lr_r, sem_p_s, sem_p_r, sem_n, sem_b,
):
    z = lax.axis_index("row")
    c = lax.axis_index("col")
    me = z * nc + c
    devs = nz * nc
    cols = pm_ref.shape[1]
    ch = x_ref.shape[1]
    per = s_lr.shape[0]
    block = devs * rows
    half = nz // 2
    other = 1 - c

    barrier = pltpu.get_barrier_semaphore()

    left, right = lax.rem(z + nz - 1, nz), lax.rem(z + 1, nz)
    for zz, cc in ((left, c), (right, c), (z, other)):
        pl.semaphore_signal(barrier, inc=1, device_id={"row": zz, "col": cc}, device_id_type=MESH)
    loads = []
    for i, (src, dst) in enumerate((
        (x_hbm, x_ref), (ng_hbm, ng_ref), (mp_hbm, mp_ref), (rm_hbm, rm_ref), (mg_hbm, mg_ref), (mo_hbm, mo_ref),
        (ag_hbm, ag_ref), (ap_hbm, ap_ref), (ab_hbm, ab_ref), (ao_hbm, ao_ref),
    )):
        loads.append(pltpu.make_async_copy(src, dst, sem_in.at[i]))
        loads[-1].start()

    def tell(n):
        pl.semaphore_signal(level.at[0, n], inc=1, device_id={"row": right, "col": c}, device_id_type=MESH)
        pl.semaphore_signal(level.at[1, n], inc=1, device_id={"row": left, "col": c}, device_id_type=MESH)

    def hear(n):
        pl.semaphore_wait(level.at[0, n], 1)
        pl.semaphore_wait(level.at[1, n], 1)

    pl.semaphore_wait(barrier, 3)
    tell(2)

    def remote(src, dst, ssem, rsem, zz, cc):
        return pltpu.make_async_remote_copy(
            src_ref=src, dst_ref=dst, send_sem=ssem, recv_sem=rsem,
            device_id={"row": zz, "col": cc}, device_id_type=MESH,
        )

    def far_first(step):
        d = half - (step + 1) // 2
        off = jnp.where(lax.rem(step, 2) == 1, d, nz - d)
        return lax.rem(z + off, nz)

    def scatter(src_at, dst, ssem, rsem):
        def one(step, carry):
            zz = far_first(step)
            for cc in range(nc):
                to = lax.rem(c + cc, nc)
                remote(src_at(zz, to), dst, ssem, rsem, zz, to).start()
            return carry

        lax.fori_loop(0, nz - 1, one, 0)
        remote(src_at(z, other), dst, ssem, rsem, z, other).start()

    def scatter_near(src_at, dst, ssem, rsem):
        def put(zz):
            for cc in range(nc):
                to = lax.rem(c + cc, nc)
                remote(src_at(zz, to), dst, ssem, rsem, zz, to).start()

        def both(d):
            put(lax.rem(z + d, nz))
            put(lax.rem(z + nz - d, nz))

        remote(src_at(z, other), dst, ssem, rsem, z, other).start()
        known = rows // 2
        for d in range(1, known + 1):
            both(d)

        def one(d, carry):
            hear(d + 1)
            tell(d + 2)
            both(d)
            return carry

        lax.fori_loop(known + 1, half, one, 0)
        hear(half + 1)
        put(lax.rem(z + half, nz))

    def landed(buf, ssem, rsem):
        every = buf.at[pl.ds(0, devs - 1)]
        return remote(every, every, ssem, rsem, z, other)

    for load in loads[:4]:
        load.wait()
    pos = lax.broadcasted_iota(jnp.int32, rm_ref.shape, 1)
    alive = jnp.where(((rm_ref[...] == 1) | (pos == 0)) & (pos < crop_ref[0]), 1.0, 0.0).astype(F32)
    km_ref[...] = jnp.where(alive > 0.0, 0.0, -1000000000.0).astype(F32)
    spot = lax.broadcasted_iota(jnp.int32, (rows, nc * cols), 1)
    want = lax.broadcasted_iota(jnp.int32, (rows, nc * cols), 0) + z * rows
    row_alive = jnp.sum(jnp.where(spot == want, alive, 0.0), axis=1, keepdims=True)
    col_alive = alive[:, :cols]
    for cc in range(1, nc):
        col_alive = jnp.where(c == cc, alive[:, cc * cols:(cc + 1) * cols], col_alive)
    pm_ref[...] = row_alive * col_alive

    def by_channel(u):
        for q in range(4):
            wt[u, q * ch:(q + 1) * ch, :] = jnp.transpose(
                mp_ref[u, :, q * ch:(q + 1) * ch].astype(F32)).astype(BF16)

    by_channel(0)

    def project(u, r):
        sl = pl.ds(pl.multiple_of(r * cols, cols), cols)
        src = x_ref if u == 0 else zb
        normed = norm_lanes(src[sl, :].astype(F32), ng_ref[u:u + 1, :]).astype(BF16)
        nrm[sl, :] = normed
        pt = dot(wt[u], normed, NT)
        mask = pm_ref[pl.ds(r, 1), :]
        left = mask * jax.nn.sigmoid(pt[ch:2 * ch]) * pt[:ch]
        right = mask * jax.nn.sigmoid(pt[3 * ch:]) * pt[2 * ch:3 * ch]
        fl[pl.ds(r, ch, stride=rows), :] = left
        fr[pl.ds(r, ch, stride=rows), :] = right
        if u == 0:
            @pl.when(lax.rem(r, 2) == 1)
            def _():
                n = 2 + r // 2
                hear(n)
                tell(n + 1)

    def send_lr(u, k):
        pair = jnp.concatenate(
            [
                fl[k * block:(k + 1) * block, :].reshape(devs, rows, cols),
                fr[k * block:(k + 1) * block, :].reshape(devs, rows, cols),
            ],
            axis=1,
        )
        s_lr[k] = pair.astype(BF16)
        r_lr[u, k, c * nz + z] = s_lr[k, me]
        go = scatter_near if u == 0 and k == 0 else scatter
        go(
            lambda zz, cc: s_lr.at[k, zz * nc + cc], r_lr.at[u, k, c * nz + z],
            sem_lr_s.at[k], sem_lr_r.at[u, k])

    def gate_row(u):
        def one(r, carry):
            sl = pl.ds(pl.multiple_of(r * cols, cols), cols)
            gate[sl, :] = jax.nn.sigmoid(dot(nrm[sl, :], mp_ref[u, :, 4 * ch:], NN))
            return carry

        lax.fori_loop(0, rows, one, 0)

    def product(u, k):
        wait = landed(r_lr.at[u, k], sem_lr_s.at[k], sem_lr_r.at[u, k])
        wait.wait_recv()
        lefts, rights = [], []
        for cc in range(nc):
            part = r_lr[u, k, cc * nz:(cc + 1) * nz].astype(F32)
            lefts.append(part[:, :rows].reshape(nz * rows, cols).astype(BF16))
            rights.append(part[:, rows:].reshape(nz * rows, cols).astype(BF16))
        left = jnp.concatenate(lefts, axis=1)
        right = jnp.concatenate(rights, axis=1)
        prod = dot(left, right, NT if u == 0 else TN)
        for cc in range(nc):
            s_p[k, cc] = prod[:, cc * cols:(cc + 1) * cols].reshape(nz, rows, cols).astype(BF16)
        r_p[u, k, me] = s_p[k, c, z]
        scatter(lambda zz, cc: s_p.at[k, cc, zz], r_p.at[u, k, me], sem_p_s.at[k], sem_p_r.at[u, k])
        wait.wait_send()

    def updated(u, r):
        sl = pl.ds(pl.multiple_of(r * cols, cols), cols)
        mixed = norm_sublanes(fl[pl.ds(r, ch, stride=rows), :], mgt[u]).astype(BF16)
        upd = dot(mixed, mo_ref[u], TN)
        src = x_ref if u == 0 else zb
        zb[sl, :] = (src[sl, :].astype(F32) + gate[sl, :] * upd).astype(BF16)

    def rows_loop(f):
        def one(r, carry):
            f(r)
            return carry

        lax.fori_loop(0, rows, one, 0)

    for u in range(2):
        rows_loop(functools.partial(project, u))
        for k in range(per):
            send_lr(u, k)
        gate_row(u)
        if u == 0:
            for load in loads[4:]:
                load.wait()
            by_channel(1)
            for w in range(2):
                mgt[w] = jnp.transpose(jnp.broadcast_to(mg_ref[w:w + 1, :], (ch, ch)))
            for q in range(4):
                apt[q * ch:(q + 1) * ch, :] = jnp.transpose(
                    ap_ref[:, q * ch:(q + 1) * ch].astype(F32)).astype(BF16)
        for k in range(per):
            product(u, k)
        for k in range(per):
            wait = landed(r_p.at[u, k], sem_p_s.at[k], sem_p_r.at[u, k])
            wait.wait_recv()
            fl[k * block:(k + 1) * block, :] = r_p[u, k].astype(F32).reshape(block, cols)
            wait.wait_send()
        rows_loop(functools.partial(updated, u))

    def normed_row(r):
        sl = pl.ds(pl.multiple_of(r * cols, cols), cols)
        normed = norm_lanes(zb[sl, :].astype(F32), ag_ref[...]).astype(BF16)
        nall[c, sl, :] = normed
        fb[pl.ds(r, HEADS, stride=rows), :] = dot(ab_ref[...], normed, NT)

    rows_loop(normed_row)
    hr = HEADS * rows
    s_b[...] = fb[:hr, :].astype(BF16)
    to = z // half
    many = nc * half // stride
    res = lax.rem(z, stride)
    slot = res * many + c * (half // stride) + lax.rem(z, half) // stride
    hops = nz // stride

    def bias_wait(count, i):
        return remote(r_b.at[pl.ds(0, count)], r_b.at[pl.ds(0, count)], sem_b.at[0, i], sem_b.at[1, i], z, other)

    for t in sorted(range(1, hops), key=lambda t: -min(t, hops - t)):
        remote(s_b, r_b.at[slot], sem_b.at[0, 0], sem_b.at[1, 0], lax.rem(z + stride * t, nz), to).start()

    @pl.when(to == c)
    def _():
        r_b[slot] = s_b[...]

    @pl.when(to != c)
    def _():
        remote(s_b, r_b.at[slot], sem_b.at[0, 0], sem_b.at[1, 0], z, other).start()

    swap = remote(nall.at[c], nall.at[c], sem_n.at[0], sem_n.at[1], z, other)
    swap.start()
    swap.wait()

    def scores_row(r):
        sl = pl.ds(pl.multiple_of(r * cols, cols), cols)
        mine_n = nall[c, sl, :]
        full = jnp.concatenate([nall[cc, sl, :] for cc in range(nc)], axis=0)
        qt = dot(apt[:ch], mine_n, NT).astype(BF16)
        gt = dot(apt[3 * ch:], mine_n, NT).astype(BF16)
        keys = dot(full, ap_ref[:, ch:2 * ch], NN).astype(BF16)
        vt[r] = dot(apt[2 * ch:3 * ch], full, NT).astype(BF16)
        sg[r] = jax.nn.sigmoid(gt.astype(F32))
        hd = ch // HEADS
        wide = []
        for h in range(HEADS):
            parts = [jnp.zeros((h * hd, cols), BF16)] if h else []
            parts.append(qt[h * hd:(h + 1) * hd])
            if h < HEADS - 1:
                parts.append(jnp.zeros(((HEADS - 1 - h) * hd, cols), BF16))
            wide.append(jnp.concatenate(parts, axis=0))
        sc[r] = dot(keys, jnp.concatenate(wide, axis=1), NN)

    @pl.when(to == c)
    def _():
        bias_wait(many - 1, 0).wait_recv()
        bias_wait(hops - 1, 0).wait_send()

    @pl.when(to != c)
    def _():
        bias_wait(many, 0).wait_recv()
        bias_wait(hops, 0).wait_send()

    group = r_b.at[pl.ds(res * many, many)]
    near = [lax.rem(z + nz + o, nz) for o in (2, 1, -1)]
    for zz in near:
        remote(group, group, sem_b.at[0, 1], sem_b.at[1, 1], zz, c).start()

    rows_loop(scores_row)
    bias_wait(len(near) * many, 1).wait()

    for kc in range(nc):
        lots = half // stride
        part = [
            r_b[q * many + kc * lots:q * many + (kc + 1) * lots].astype(F32) for q in range(stride)
        ]
        for h in range(HEADS):
            tile = jnp.stack([p[:, h * rows:(h + 1) * rows] for p in part], axis=1).reshape(half * rows, cols)
            tile = tile + km_ref[:, kc * cols:(kc + 1) * cols]
            bt[kc * cols:(kc + 1) * cols, h * cols:(h + 1) * cols] = jnp.transpose(tile)

    hd = ch // HEADS
    scale = 1.0 / float(hd) ** 0.5

    def attend_row(r):
        sl = pl.ds(pl.multiple_of(r * cols, cols), cols)
        score = sc[r] * scale + bt[...]
        top = jnp.max(score, axis=0, keepdims=True)
        e = jnp.exp(score - top)
        inv = 1.0 / jnp.sum(e, axis=0, keepdims=True)
        got = dot(vt[r], e.astype(BF16), NN)
        parts = []
        for h in range(HEADS):
            lanes = slice(h * cols, (h + 1) * cols)
            parts.append(got[h * hd:(h + 1) * hd, lanes] * inv[:, lanes])
        gated = (sg[r] * jnp.concatenate(parts, axis=0)).astype(BF16)
        out_ref[sl, :] = (zb[sl, :].astype(F32) + dot(gated, ao_ref[...], TN)).astype(BF16)

    rows_loop(attend_row)


def solution(mesh):
    nz, nc = mesh.shape["row"], mesh.shape["col"]
    devs = nz * nc

    def local(pair_rep, residue_mask, crop_length, norm_gain, mult_proj, mixed_gain, mult_out, att_gain, att_proj,
              att_bias, att_out):
        rows, cols, ch = pair_rep.shape
        per = ch // devs
        half = nz // 2
        area = rows * cols
        vmem = pltpu.VMEM
        out = pl.pallas_call(
            functools.partial(kernel, nz, nc, rows, 4),
            out_shape=jax.ShapeDtypeStruct((area, ch), BF16),
            in_specs=[pl.BlockSpec(memory_space=pltpu.SMEM)] + [pl.BlockSpec(memory_space=pl.ANY)] * 10,
            out_specs=pl.BlockSpec(memory_space=vmem),
            scratch_shapes=[
                vmem((1, nc * cols), jnp.int32),
                vmem((area, ch), BF16),
                vmem(norm_gain.shape, F32),
                vmem(mult_proj.shape, BF16),
                vmem(mixed_gain.shape, F32),
                vmem(mult_out.shape, BF16),
                vmem((1, ch), F32),
                vmem(att_proj.shape, BF16),
                vmem((HEADS, ch), BF16),
                vmem(att_out.shape, BF16),
                pltpu.SemaphoreType.DMA((10,)),
                vmem((rows, cols), F32),
                vmem((1, nc * cols), F32),
                vmem((2, 4 * ch, ch), BF16),
                vmem((2, ch, ch), F32),
                vmem((4 * ch, ch), BF16),
                vmem((area, ch), BF16),
                vmem((area, ch), F32),
                vmem((area, ch), BF16),
                vmem((ch * rows, cols), F32),
                vmem((ch * rows, cols), F32),
                vmem((per, devs, 2 * rows, cols), BF16),
                vmem((2, per, devs, 2 * rows, cols), BF16),
                vmem((per, nc, nz, rows, cols), BF16),
                vmem((2, per, devs, rows, cols), BF16),
                vmem((nc, area, ch), BF16),
                vmem((HEADS * rows, cols), F32),
                vmem((HEADS * rows, cols), BF16),
                vmem((nc * half, HEADS * rows, cols), BF16),
                vmem((nc * cols, HEADS * cols), F32),
                vmem((rows, nc * cols, HEADS * cols), F32),
                vmem((rows, ch, nc * cols), BF16),
                vmem((rows, ch, cols), F32),
                pltpu.SemaphoreType.REGULAR((2, half + 2)),
                pltpu.SemaphoreType.DMA((per,)),
                pltpu.SemaphoreType.DMA((2, per)),
                pltpu.SemaphoreType.DMA((per,)),
                pltpu.SemaphoreType.DMA((2, per)),
                pltpu.SemaphoreType.DMA((2,)),
                pltpu.SemaphoreType.DMA((2, 2)),
            ],
            compiler_params=pltpu.CompilerParams(
                collective_id=1, has_side_effects=True, vmem_limit_bytes=62 * 1024 * 1024
            ),
            name="triangle",
        )(
            crop_length, residue_mask.reshape(1, nc * cols), pair_rep.reshape(area, ch), norm_gain, mult_proj,
            mixed_gain, mult_out, att_gain.reshape(1, ch), att_proj, att_bias.T, att_out,
        )
        return out.reshape(rows, cols, ch)

    return jax.shard_map(
        local,
        mesh=mesh,
        in_specs=(P(("groups", "row"), "col", None), P("groups"), P("groups")) + (P(),) * 8,
        out_specs=P(("groups", "row"), "col", None),
        check_vma=False,
    )
```

```python
import functools

import jax
import jax.numpy as jnp
from jax import lax
from jax.experimental import pallas as pl
from jax.experimental.pallas import tpu as pltpu
from jax.sharding import PartitionSpec as P

HEADS = 4
EPSILON = 1e-05
MESH = pl.DeviceIdType.MESH
F32 = jnp.float32
BF16 = jnp.bfloat16
NN = (((1,), (0,)), ((), ()))
NT = (((1,), (1,)), ((), ()))
TN = (((0,), (0,)), ((), ()))


def dot(a, b, dims):
    return lax.dot_general(a, b, dims, preferred_element_type=F32)


def norm_lanes(v, gain):
    mean = jnp.mean(v, axis=-1, keepdims=True)
    cen = v - mean
    var = jnp.mean(cen * cen, axis=-1, keepdims=True)
    return cen * lax.rsqrt(var + EPSILON) * gain


def norm_sublanes(v, gain):
    mean = jnp.mean(v, axis=0, keepdims=True)
    cen = v - mean
    var = jnp.mean(cen * cen, axis=0, keepdims=True)
    return cen * lax.rsqrt(var + EPSILON) * gain


def kernel(
    nz, nc, rows, stride, crop_ref, rm_hbm, x_hbm, ng_hbm, mp_hbm, mg_hbm, mo_hbm, ag_hbm, ap_hbm, ab_hbm, ao_hbm,
    out_ref,
    rm_ref, x_ref, ng_ref, mp_ref, mg_ref, mo_ref, ag_ref, ap_ref, ab_ref, ao_ref, sem_in,
    pm_ref, km_ref, wt, mgt, apt, nrm, gate, zb, fl, fr, fp, s_lr, r_lr, s_l2, r_l2, s_p, r_p, s_q, r_q, nall, fb, s_b, r_b, bt, sc, vt, sg,
    level, sem_lr, sem_l2, sem_p, sem_q, sem_n, sem_bf, sem_b,
):
    z = lax.axis_index("row")
    c = lax.axis_index("col")
    me = z * nc + c
    devs = nz * nc
    cols = pm_ref.shape[1]
    ch = x_ref.shape[1]
    per = s_lr.shape[0]
    block = devs * rows
    half = nz // 2
    other = 1 - c

    barrier = pltpu.get_barrier_semaphore()

    left, right = lax.rem(z + nz - 1, nz), lax.rem(z + 1, nz)
    for zz, cc in ((left, c), (right, c), (left, other), (right, other), (z, other)):
        pl.semaphore_signal(barrier, inc=1, device_id={"row": zz, "col": cc}, device_id_type=MESH)
    loads = []
    for i, (src, dst) in enumerate((
        (x_hbm, x_ref), (ng_hbm, ng_ref), (mp_hbm, mp_ref), (rm_hbm, rm_ref), (mg_hbm, mg_ref), (mo_hbm, mo_ref),
        (ag_hbm, ag_ref), (ap_hbm, ap_ref), (ab_hbm, ab_ref), (ao_hbm, ao_ref),
    )):
        loads.append(pltpu.make_async_copy(src, dst, sem_in.at[i]))
        loads[-1].start()

    def tell(n):
        up, down = lax.rem(z + 2 ** n, nz), lax.rem(z + nz - 2 ** n, nz)
        pl.semaphore_signal(level.at[0, n], inc=1, device_id={"row": up, "col": c}, device_id_type=MESH)
        pl.semaphore_signal(level.at[1, n], inc=1, device_id={"row": down, "col": c}, device_id_type=MESH)

    def hear(n):
        pl.semaphore_wait(level.at[0, n - 1], 1)
        pl.semaphore_wait(level.at[1, n - 1], 1)

    pl.semaphore_wait(barrier, 5)
    tell(0)

    def remote(src, dst, ssem, rsem, zz, cc):
        return pltpu.make_async_remote_copy(
            src_ref=src, dst_ref=dst, send_sem=ssem, recv_sem=rsem,
            device_id={"row": zz, "col": cc}, device_id_type=MESH,
        )

    def far_first(step):
        d = half - (step + 1) // 2
        off = jnp.where(lax.rem(step, 2) == 1, d, nz - d)
        return lax.rem(z + off, nz)

    def scatter(src_at, dst, ssem, rsem):
        def one(step, carry):
            zz = far_first(step)
            for cc in range(nc):
                to = lax.rem(c + cc, nc)
                remote(src_at(zz, to), dst, ssem, rsem, zz, to).start()
            return carry

        lax.fori_loop(0, nz - 1, one, 0)
        remote(src_at(z, other), dst, ssem, rsem, z, other).start()

    def ring(src_at, dst, ssem, rsem, near, far):
        def put(zz):
            for cc in range(nc):
                to = lax.rem(c + cc, nc)
                remote(src_at(zz, to), dst, ssem, rsem, zz, to).start()

        def both(i, carry):
            d = far - i
            put(lax.rem(z + d, nz))
            put(lax.rem(z + nz - d, nz))
            return carry

        if near == 1:
            remote(src_at(z, other), dst, ssem, rsem, z, other).start()
        if far == half:
            put(lax.rem(z + half, nz))
            far -= 1
        lax.fori_loop(0, far + 1 - near, both, 0)

    def landed(buf, ssem, rsem):
        every = buf.at[pl.ds(0, devs - 1)]
        return remote(every, every, ssem, rsem, z, other)

    for load in loads[:4]:
        load.wait()
    pos = lax.broadcasted_iota(jnp.int32, rm_ref.shape, 1)
    alive = jnp.where(((rm_ref[...] == 1) | (pos == 0)) & (pos < crop_ref[0]), 1.0, 0.0).astype(F32)
    km_ref[...] = jnp.where(alive > 0.0, 0.0, -1000000000.0).astype(F32)
    spot = lax.broadcasted_iota(jnp.int32, (rows, nc * cols), 1)
    want = lax.broadcasted_iota(jnp.int32, (rows, nc * cols), 0) + z * rows
    row_alive = jnp.sum(jnp.where(spot == want, alive, 0.0), axis=1, keepdims=True)
    col_alive = alive[:, :cols]
    for cc in range(1, nc):
        col_alive = jnp.where(c == cc, alive[:, cc * cols:(cc + 1) * cols], col_alive)
    pm_ref[...] = row_alive * col_alive

    def by_channel(u):
        for q in range(4):
            wt[u, q * ch:(q + 1) * ch, :] = jnp.transpose(
                mp_ref[u, :, q * ch:(q + 1) * ch].astype(F32)).astype(BF16)

    by_channel(0)

    hr = rows // 2

    def project(u, r, hf=0):
        sl = pl.ds(pl.multiple_of(r * cols, cols), cols)
        src = x_ref if u == 0 else zb
        normed = norm_lanes(src[sl, :].astype(F32), ng_ref[u:u + 1, :]).astype(BF16)
        nrm[sl, :] = normed
        pt = dot(wt[u], normed, NT)
        mask = pm_ref[pl.ds(r, 1), :]
        left = mask * jax.nn.sigmoid(pt[ch:2 * ch]) * pt[:ch]
        right = mask * jax.nn.sigmoid(pt[3 * ch:]) * pt[2 * ch:3 * ch]
        if u == 0:
            fl[pl.ds(r, ch, stride=rows), :] = left
            fr[pl.ds(r, ch, stride=rows), :] = right
        elif hf == 0:
            fl[pl.ds(r, ch, stride=rows), :] = left
            fl[pl.ds(r + hr, ch, stride=rows), :] = right
        else:
            fr[pl.ds(r, ch, stride=rows), :] = left
            fr[pl.ds(r - hr, ch, stride=rows), :] = right

    def pack(k):
        pair = jnp.concatenate(
            [
                fl[k * block:(k + 1) * block, :].reshape(devs, rows, cols),
                fr[k * block:(k + 1) * block, :].reshape(devs, rows, cols),
            ],
            axis=1,
        )
        s_lr[k] = pair.astype(BF16)
        r_lr[k, c * nz + z] = s_lr[k, me]

    def send_first(k, near, far):
        ring(lambda zz, cc: s_lr.at[k, zz * nc + cc], r_lr.at[k, c * nz + z], sem_lr.at[0, k], sem_lr.at[1, k], near, far)

    def send_second(hf, k):
        src = fl if hf == 0 else fr
        s_l2[hf, k] = src[k * block:(k + 1) * block, :].reshape(devs, rows, cols).astype(BF16)
        r_l2[hf, k, c * nz + z] = s_l2[hf, k, me]
        scatter(
            lambda zz, cc: s_l2.at[hf, k, zz * nc + cc], r_l2.at[hf, k, c * nz + z],
            sem_l2.at[0, hf, k], sem_l2.at[1, hf, k])

    def gate_row(u, r):
        sl = pl.ds(pl.multiple_of(r * cols, cols), cols)
        gate[sl, :] = jax.nn.sigmoid(dot(nrm[sl, :], mp_ref[u, :, 4 * ch:], NN))

    def product(u, k):
        lefts, rights = [], []
        if u == 0:
            landed(r_lr.at[k], sem_lr.at[0, k], sem_lr.at[1, k]).wait_recv()
            for cc in range(nc):
                part = r_lr[k, cc * nz:(cc + 1) * nz].astype(F32)
                lefts.append(part[:, :rows].reshape(nz * rows, cols).astype(BF16))
                rights.append(part[:, rows:].reshape(nz * rows, cols).astype(BF16))
        else:
            for hf in range(2):
                landed(r_l2.at[hf, k], sem_l2.at[0, hf, k], sem_l2.at[1, hf, k]).wait_recv()
            low = lax.broadcasted_iota(jnp.int32, (nz, rows, cols), 1) < hr
            for cc in range(nc):
                first = r_l2[0, k, cc * nz:(cc + 1) * nz].astype(F32)
                last = r_l2[1, k, cc * nz:(cc + 1) * nz].astype(F32)
                lefts.append(jnp.where(low, first, last).reshape(nz * rows, cols).astype(BF16))
                turned = pltpu.roll(jnp.where(low, last, first), hr, 1)
                rights.append(turned.reshape(nz * rows, cols).astype(BF16))
        left = jnp.concatenate(lefts, axis=1)
        right = jnp.concatenate(rights, axis=1)
        prod = dot(left, right, NT if u == 0 else TN)
        tiles = [prod[:, cc * cols:(cc + 1) * cols].reshape(nz, rows, cols) for cc in range(nc)]
        if k == 0:
            for cc in range(nc):
                s_p[u, cc] = tiles[cc].astype(BF16)
            r_p[u, me] = s_p[u, c, z]
            scatter(lambda zz, cc: s_p.at[u, cc, zz], r_p.at[u, me], sem_p.at[0, u], sem_p.at[1, u])
            return
        for hf in range(2):
            for cc in range(nc):
                s_q[u, hf, cc] = tiles[cc][:, hf * hr:(hf + 1) * hr].astype(BF16)
            r_q[u, hf, me] = s_q[u, hf, c, z]
            scatter(
                lambda zz, cc: s_q.at[u, hf, cc, zz], r_q.at[u, hf, me], sem_q.at[0, u, hf], sem_q.at[1, u, hf])

    def returned(u, hf):
        if hf == 0:
            landed(r_p.at[u], sem_p.at[0, u], sem_p.at[1, u]).wait_recv()
            fp[:block, :] = r_p[u].astype(F32).reshape(block, cols)
        landed(r_q.at[u, hf], sem_q.at[0, u, hf], sem_q.at[1, u, hf]).wait_recv()
        view = fp.reshape(ch, rows, cols)
        view[devs:, hf * hr:(hf + 1) * hr, :] = r_q[u, hf].astype(F32)

    def updated(u, r):
        sl = pl.ds(pl.multiple_of(r * cols, cols), cols)
        mixed = norm_sublanes(fp[pl.ds(r, ch, stride=rows), :], mgt[u]).astype(BF16)
        upd = dot(mixed, mo_ref[u], TN)
        src = x_ref if u == 0 else zb
        zb[sl, :] = (src[sl, :].astype(F32) + gate[sl, :] * upd).astype(BF16)

    def rows_loop(f, lo=0, hi=rows, step=2):
        def some(i, carry):
            for t in range(step):
                f(lo + i * step + t)
            return carry

        lax.fori_loop(0, (hi - lo) // step, some, 0)

    def first_row(r):
        project(0, r)

    rows_loop(first_row, 0, hr)
    hear(1)
    tell(1)
    rows_loop(first_row, hr, rows)
    pack(0)
    hear(2)
    tell(2)
    send_first(0, 1, 4)
    pack(1)
    send_first(1, 1, 4)
    for load in loads[4:]:
        load.wait()
    by_channel(1)
    hear(3)
    tell(3)
    send_first(0, 5, 8)
    send_first(1, 5, 8)
    rows_loop(functools.partial(gate_row, 0))
    hear(4)
    send_first(0, 9, half)
    send_first(1, 9, half)
    for w in range(2):
        mgt[w] = jnp.transpose(jnp.broadcast_to(mg_ref[w:w + 1, :], (ch, ch)))
    for q in range(4):
        apt[q * ch:(q + 1) * ch, :] = jnp.transpose(
            ap_ref[:, q * ch:(q + 1) * ch].astype(F32)).astype(BF16)
    for k in range(per):
        product(0, k)
    for hf in range(2):
        returned(0, hf)

        def both_steps(r, hf=hf):
            updated(0, r)
            project(1, r, hf)

        rows_loop(both_steps, hf * hr, (hf + 1) * hr)
        for k in range(per):
            send_second(hf, k)
    rows_loop(functools.partial(gate_row, 1))
    for k in range(per):
        product(1, k)

    def normed_row(r):
        sl = pl.ds(pl.multiple_of(r * cols, cols), cols)
        normed = norm_lanes(zb[sl, :].astype(F32), ag_ref[...]).astype(BF16)
        nall[c, sl, :] = normed
        fb[pl.ds(r, HEADS, stride=rows), :] = dot(ab_ref[...], normed, NT)

    for hf in range(2):
        returned(1, hf)

        def last_steps(r):
            updated(1, r)
            normed_row(r)

        rows_loop(last_steps, hf * hr, (hf + 1) * hr)
    s_b[...] = fb[...].astype(BF16)
    to = z // half
    lots = half // stride
    many = nc * lots
    res = lax.rem(z, stride)
    turn = lax.rem(z, half) // stride
    slot = res * many + turn * nc + c
    hops = nz // stride

    def bias_wait(count, ssem, rsem):
        return remote(r_b.at[pl.ds(0, count)], r_b.at[pl.ds(0, count)], ssem, rsem, z, other)

    for t in sorted(range(1, hops), key=lambda t: -min(t, hops - t)):
        remote(s_b, r_b.at[slot], sem_b.at[0], sem_bf.at[turn], lax.rem(z + stride * t, nz), to).start()

    @pl.when(to == c)
    def _():
        r_b[slot] = s_b[...]

    @pl.when(to != c)
    def _():
        remote(s_b, r_b.at[slot], sem_b.at[0], sem_bf.at[turn], z, other).start()

    swap = remote(nall.at[c], nall.at[c], sem_n.at[0], sem_n.at[1], z, other)
    swap.start()

    def scores_row(r):
        sl = pl.ds(pl.multiple_of(r * cols, cols), cols)
        mine_n = nall[c, sl, :]
        full = jnp.concatenate([nall[cc, sl, :] for cc in range(nc)], axis=0)
        qt = dot(apt[:ch], mine_n, NT).astype(BF16)
        gt = dot(apt[3 * ch:], mine_n, NT).astype(BF16)
        keys = dot(full, ap_ref[:, ch:2 * ch], NN).astype(BF16)
        vt[r] = dot(apt[2 * ch:3 * ch], full, NT).astype(BF16)
        sg[r] = jax.nn.sigmoid(gt.astype(F32))
        hd = ch // HEADS
        wide = []
        for h in range(HEADS):
            parts = [jnp.zeros((h * hd, cols), BF16)] if h else []
            parts.append(qt[h * hd:(h + 1) * hd])
            if h < HEADS - 1:
                parts.append(jnp.zeros(((HEADS - 1 - h) * hd, cols), BF16))
            wide.append(jnp.concatenate(parts, axis=0))
        sc[r] = dot(keys, jnp.concatenate(wide, axis=1), NN)

    swap.wait()
    rows_loop(scores_row)

    near = [lax.rem(z + nz + o, nz) for o in (2, 1, -1)]
    for t in sorted(range(hops), key=lambda t: min(t, hops - t)):
        zz = lax.rem(z + stride * t, nz)
        src_turn = lax.rem(zz, half) // stride

        @pl.when(zz // half == c)
        def _(t=t, src_turn=src_turn):
            bias_wait(nc - 1 if t == 0 else nc, sem_b.at[0], sem_bf.at[src_turn]).wait_recv()
            group = r_b.at[pl.ds(res * many + src_turn * nc, nc)]
            for beside in near:
                remote(group, group, sem_b.at[1], sem_b.at[2], beside, c).start()

    bias_wait(len(near) * many, sem_b.at[1], sem_b.at[2]).wait()

    for kc in range(nc):
        part = [
            jnp.stack([r_b[q * many + m * nc + kc] for m in range(lots)]).astype(F32) for q in range(stride)
        ]
        for h in range(HEADS):
            tile = jnp.stack([p[:, h * rows:(h + 1) * rows] for p in part], axis=1).reshape(half * rows, cols)
            tile = tile + km_ref[:, kc * cols:(kc + 1) * cols]
            bt[kc * cols:(kc + 1) * cols, h * cols:(h + 1) * cols] = jnp.transpose(tile)

    hd = ch // HEADS
    scale = 1.0 / float(hd) ** 0.5

    def attend_row(r):
        sl = pl.ds(pl.multiple_of(r * cols, cols), cols)
        score = sc[r] * scale + bt[...]
        top = jnp.max(score, axis=0, keepdims=True)
        e = jnp.exp(score - top)
        inv = 1.0 / jnp.sum(e, axis=0, keepdims=True)
        got = dot(vt[r], e.astype(BF16), NN)
        parts = []
        for h in range(HEADS):
            lanes = slice(h * cols, (h + 1) * cols)
            parts.append(got[h * hd:(h + 1) * hd, lanes] * inv[:, lanes])
        gated = (sg[r] * jnp.concatenate(parts, axis=0)).astype(BF16)
        out_ref[sl, :] = (zb[sl, :].astype(F32) + dot(gated, ao_ref[...], TN)).astype(BF16)

    rows_loop(attend_row)

    for k in range(per):
        landed(r_lr.at[k], sem_lr.at[0, k], sem_lr.at[1, k]).wait_send()
        landed(r_p.at[k], sem_p.at[0, k], sem_p.at[1, k]).wait_send()
        for hf in range(2):
            landed(r_l2.at[hf, k], sem_l2.at[0, hf, k], sem_l2.at[1, hf, k]).wait_send()
            landed(r_q.at[k, hf], sem_q.at[0, k, hf], sem_q.at[1, k, hf]).wait_send()

    @pl.when(to == c)
    def _():
        bias_wait(hops - 1, sem_b.at[0], sem_b.at[2]).wait_send()

    @pl.when(to != c)
    def _():
        bias_wait(hops, sem_b.at[0], sem_b.at[2]).wait_send()


def solution(mesh):
    nz, nc = mesh.shape["row"], mesh.shape["col"]
    devs = nz * nc

    def local(pair_rep, residue_mask, crop_length, norm_gain, mult_proj, mixed_gain, mult_out, att_gain, att_proj,
              att_bias, att_out):
        rows, cols, ch = pair_rep.shape
        per = ch // devs
        half = nz // 2
        area = rows * cols
        vmem = pltpu.VMEM
        out = pl.pallas_call(
            functools.partial(kernel, nz, nc, rows, 4),
            out_shape=jax.ShapeDtypeStruct((area, ch), BF16),
            in_specs=[pl.BlockSpec(memory_space=pltpu.SMEM)] + [pl.BlockSpec(memory_space=pl.ANY)] * 10,
            out_specs=pl.BlockSpec(memory_space=vmem),
            scratch_shapes=[
                vmem((1, nc * cols), jnp.int32),
                vmem((area, ch), BF16),
                vmem(norm_gain.shape, F32),
                vmem(mult_proj.shape, BF16),
                vmem(mixed_gain.shape, F32),
                vmem(mult_out.shape, BF16),
                vmem((1, ch), F32),
                vmem(att_proj.shape, BF16),
                vmem((HEADS, ch), BF16),
                vmem(att_out.shape, BF16),
                pltpu.SemaphoreType.DMA((10,)),
                vmem((rows, cols), F32),
                vmem((1, nc * cols), F32),
                vmem((2, 4 * ch, ch), BF16),
                vmem((2, ch, ch), F32),
                vmem((4 * ch, ch), BF16),
                vmem((area, ch), BF16),
                vmem((area, ch), F32),
                vmem((area, ch), BF16),
                vmem((ch * rows, cols), F32),
                vmem((ch * rows, cols), F32),
                vmem((ch * rows, cols), F32),
                vmem((per, devs, 2 * rows, cols), BF16),
                vmem((per, devs, 2 * rows, cols), BF16),
                vmem((2, per, devs, rows, cols), BF16),
                vmem((2, per, devs, rows, cols), BF16),
                vmem((2, nc, nz, rows, cols), BF16),
                vmem((2, devs, rows, cols), BF16),
                vmem((2, 2, nc, nz, rows // 2, cols), BF16),
                vmem((2, 2, devs, rows // 2, cols), BF16),
                vmem((nc, area, ch), BF16),
                vmem((HEADS * rows, cols), F32),
                vmem((HEADS * rows, cols), BF16),
                vmem((nc * half, HEADS * rows, cols), BF16),
                vmem((nc * cols, HEADS * cols), F32),
                vmem((rows, nc * cols, HEADS * cols), F32),
                vmem((rows, ch, nc * cols), BF16),
                vmem((rows, ch, cols), F32),
                pltpu.SemaphoreType.REGULAR((2, 4)),
                pltpu.SemaphoreType.DMA((2, per)),
                pltpu.SemaphoreType.DMA((2, 2, per)),
                pltpu.SemaphoreType.DMA((2, 2)),
                pltpu.SemaphoreType.DMA((2, 2, 2)),
                pltpu.SemaphoreType.DMA((2,)),
                pltpu.SemaphoreType.DMA((half // 4,)),
                pltpu.SemaphoreType.DMA((3,)),
            ],
            compiler_params=pltpu.CompilerParams(
                collective_id=1, has_side_effects=True, vmem_limit_bytes=62 * 1024 * 1024
            ),
            name="triangle",
        )(
            crop_length, residue_mask.reshape(1, nc * cols), pair_rep.reshape(area, ch), norm_gain, mult_proj,
            mixed_gain, mult_out, att_gain.reshape(1, ch), att_proj, att_bias.T, att_out,
        )
        return out.reshape(rows, cols, ch)

    return jax.shard_map(
        local,
        mesh=mesh,
        in_specs=(P(("groups", "row"), "col", None), P("groups"), P("groups")) + (P(),) * 8,
        out_specs=P(("groups", "row"), "col", None),
        check_vma=False,
    )
```

```python
import functools

import jax
import jax.numpy as jnp
from jax import lax
from jax.experimental import pallas as pl
from jax.experimental.pallas import tpu as pltpu
from jax.sharding import PartitionSpec as P

HEADS = 4
EPSILON = 1e-05
MESH = pl.DeviceIdType.MESH
F32 = jnp.float32
BF16 = jnp.bfloat16
NN = (((1,), (0,)), ((), ()))
NT = (((1,), (1,)), ((), ()))
TN = (((0,), (0,)), ((), ()))


def dot(a, b, dims):
    return lax.dot_general(a, b, dims, preferred_element_type=F32)


def norm_lanes(v, gain):
    mean = jnp.mean(v, axis=-1, keepdims=True)
    cen = v - mean
    var = jnp.mean(cen * cen, axis=-1, keepdims=True)
    return cen * lax.rsqrt(var + EPSILON) * gain


def norm_sublanes(v, gain):
    mean = jnp.mean(v, axis=0, keepdims=True)
    cen = v - mean
    var = jnp.mean(cen * cen, axis=0, keepdims=True)
    return cen * lax.rsqrt(var + EPSILON) * gain


def kernel(
    nz, nc, rows, stride, reach, crop_ref, rm_hbm, x_hbm, ng_hbm, mp_hbm, mg_hbm, mo_hbm, ag_hbm, ap_hbm, ab_hbm, ao_hbm,
    out_hbm,
    rm_ref, x_ref, ng_ref, mp_ref, mg_ref, mo_ref, ag_ref, ap_ref, ab_ref, ao_ref, sem_in,
    pm_ref, km_ref, wt, mgt, apt, nrm, gate, zb, fl, fr, fp, s_lr, r_lr, s_l2, r_l2, s_p, r_p, s_q, r_q, nall, fb, s_b, r_b, bt, sc, vt, sg, ob,
    level, sem_lr, sem_l2, sem_p, sem_q, sem_n, sem_bf, sem_bs, sem_b, sem_o,
):
    z = lax.axis_index("row")
    c = lax.axis_index("col")
    me = z * nc + c
    devs = nz * nc
    cols = pm_ref.shape[1]
    ch = x_ref.shape[1]
    hd = ch // HEADS
    per = s_lr.shape[0]
    block = devs * rows
    half = nz // 2
    other = 1 - c

    barrier = pltpu.get_barrier_semaphore()

    for d in range(1, reach + 1):
        for zz in (lax.rem(z + d, nz), lax.rem(z + nz - d, nz)):
            for cc in (c, other):
                pl.semaphore_signal(barrier, inc=1, device_id={"row": zz, "col": cc}, device_id_type=MESH)
    pl.semaphore_signal(barrier, inc=1, device_id={"row": z, "col": other}, device_id_type=MESH)
    loads = []
    for i, (src, dst) in enumerate((
        (x_hbm, x_ref), (ng_hbm, ng_ref), (mp_hbm, mp_ref), (rm_hbm, rm_ref), (mg_hbm, mg_ref), (mo_hbm, mo_ref),
        (ag_hbm, ag_ref), (ap_hbm, ap_ref), (ab_hbm, ab_ref), (ao_hbm, ao_ref),
    )):
        loads.append(pltpu.make_async_copy(src, dst, sem_in.at[i]))
        loads[-1].start()

    def tell(d, n):
        up, down = lax.rem(z + d, nz), lax.rem(z + nz - d, nz)
        pl.semaphore_signal(level.at[0, n], inc=1, device_id={"row": up, "col": c}, device_id_type=MESH)
        pl.semaphore_signal(level.at[1, n], inc=1, device_id={"row": down, "col": c}, device_id_type=MESH)

    def hear(n):
        pl.semaphore_wait(level.at[0, n], 1)
        pl.semaphore_wait(level.at[1, n], 1)

    def remote(src, dst, ssem, rsem, zz, cc):
        return pltpu.make_async_remote_copy(
            src_ref=src, dst_ref=dst, send_sem=ssem, recv_sem=rsem,
            device_id={"row": zz, "col": cc}, device_id_type=MESH,
        )

    def ring(src_at, dst, ssem, rsem, near, far):
        def put(zz):
            remote(src_at(zz, c), dst, ssem, rsem, zz, c).start()
            remote(src_at(zz, other), dst, ssem, rsem, zz, other).start()

        def both(i, carry):
            up, down = z + far - i, z - far + i
            put(jnp.where(up >= nz, up - nz, up))
            put(jnp.where(down < 0, down + nz, down))
            return carry

        if far == half:
            put(lax.rem(z + half, nz))
            far -= 1
        lax.fori_loop(0, far + 1 - near, both, 0)
        if near == 1:
            remote(src_at(z, other), dst, ssem, rsem, z, other).start()

    def scatter(src_at, dst, ssem, rsem):
        ring(src_at, dst, ssem, rsem, 1, half)

    def landed(buf, ssem, rsem):
        every = buf.at[pl.ds(0, devs - 1)]
        return remote(every, every, ssem, rsem, z, other)

    for load in loads[:4]:
        load.wait()
    pos = lax.broadcasted_iota(jnp.int32, rm_ref.shape, 1)
    alive = jnp.where(((rm_ref[...] == 1) | (pos == 0)) & (pos < crop_ref[0]), 1.0, 0.0).astype(F32)
    km_ref[...] = jnp.where(alive > 0.0, 0.0, -1000000000.0).astype(F32)
    spot = lax.broadcasted_iota(jnp.int32, (rows, nc * cols), 1)
    want = lax.broadcasted_iota(jnp.int32, (rows, nc * cols), 0) + z * rows
    row_alive = jnp.sum(jnp.where(spot == want, alive, 0.0), axis=1, keepdims=True)
    col_alive = alive[:, :cols]
    for cc in range(1, nc):
        col_alive = jnp.where(c == cc, alive[:, cc * cols:(cc + 1) * cols], col_alive)
    pm_ref[...] = row_alive * col_alive

    def by_channel(u):
        for q in range(4):
            wt[u, q * ch:(q + 1) * ch, :] = jnp.transpose(
                mp_ref[u, :, q * ch:(q + 1) * ch].astype(F32)).astype(BF16)

    by_channel(0)

    hr = rows // 2

    def project(u, r, hf=0):
        sl = pl.ds(pl.multiple_of(r * cols, cols), cols)
        src = x_ref if u == 0 else zb
        normed = norm_lanes(src[sl, :].astype(F32), ng_ref[u:u + 1, :]).astype(BF16)
        nrm[sl, :] = normed
        pt = dot(wt[u], normed, NT)
        mask = pm_ref[pl.ds(r, 1), :]
        left = mask * jax.nn.sigmoid(pt[ch:2 * ch]) * pt[:ch]
        right = mask * jax.nn.sigmoid(pt[3 * ch:]) * pt[2 * ch:3 * ch]
        if u == 0:
            fl[pl.ds(r, ch, stride=rows), :] = left
            fr[pl.ds(r, ch, stride=rows), :] = right
        elif hf == 0:
            fl[pl.ds(r, ch, stride=rows), :] = left
            fl[pl.ds(r + hr, ch, stride=rows), :] = right
        else:
            fr[pl.ds(r, ch, stride=rows), :] = left
            fr[pl.ds(r - hr, ch, stride=rows), :] = right

    def pack(k):
        pair = jnp.concatenate(
            [
                fl[k * block:(k + 1) * block, :].reshape(devs, rows, cols),
                fr[k * block:(k + 1) * block, :].reshape(devs, rows, cols),
            ],
            axis=1,
        )
        s_lr[k] = pair.astype(BF16)
        r_lr[k, c * nz + z] = s_lr[k, me]

    def send_first(k, near, far):
        ring(lambda zz, cc: s_lr.at[k, zz * nc + cc], r_lr.at[k, c * nz + z], sem_lr.at[0, k], sem_lr.at[1, k], near, far)

    def send_second(hf, k):
        src = fl if hf == 0 else fr
        s_l2[hf, k] = src[k * block:(k + 1) * block, :].reshape(devs, rows, cols).astype(BF16)
        r_l2[hf, k, c * nz + z] = s_l2[hf, k, me]
        scatter(
            lambda zz, cc: s_l2.at[hf, k, zz * nc + cc], r_l2.at[hf, k, c * nz + z],
            sem_l2.at[0, hf, k], sem_l2.at[1, hf, k])

    def gate_row(u, r):
        sl = pl.ds(pl.multiple_of(r * cols, cols), cols)
        gate[sl, :] = jax.nn.sigmoid(dot(nrm[sl, :], mp_ref[u, :, 4 * ch:], NN))

    def product(u, k):
        lefts, rights = [], []
        if u == 0:
            landed(r_lr.at[k], sem_lr.at[0, k], sem_lr.at[1, k]).wait_recv()
            for cc in range(nc):
                part = r_lr[k, cc * nz:(cc + 1) * nz].astype(F32)
                lefts.append(part[:, :rows].reshape(nz * rows, cols).astype(BF16))
                rights.append(part[:, rows:].reshape(nz * rows, cols).astype(BF16))
        else:
            for hf in range(2):
                landed(r_l2.at[hf, k], sem_l2.at[0, hf, k], sem_l2.at[1, hf, k]).wait_recv()
            low = lax.broadcasted_iota(jnp.int32, (nz, rows, cols), 1) < hr
            for cc in range(nc):
                first = r_l2[0, k, cc * nz:(cc + 1) * nz].astype(F32)
                last = r_l2[1, k, cc * nz:(cc + 1) * nz].astype(F32)
                lefts.append(jnp.where(low, first, last).reshape(nz * rows, cols).astype(BF16))
                turned = pltpu.roll(jnp.where(low, last, first), hr, 1)
                rights.append(turned.reshape(nz * rows, cols).astype(BF16))
        left = jnp.concatenate(lefts, axis=1)
        right = jnp.concatenate(rights, axis=1)
        prod = dot(left, right, NT if u == 0 else TN)
        tiles = [prod[:, cc * cols:(cc + 1) * cols].reshape(nz, rows, cols) for cc in range(nc)]
        if u or k == 0:
            n = u + k
            for cc in range(nc):
                s_p[n, cc] = tiles[cc].astype(BF16)
            r_p[n, me] = s_p[n, c, z]
            scatter(lambda zz, cc: s_p.at[n, cc, zz], r_p.at[n, me], sem_p.at[0, n], sem_p.at[1, n])
            return
        for hf in range(2):
            for cc in range(nc):
                s_q[hf, cc] = tiles[cc][:, hf * hr:(hf + 1) * hr].astype(BF16)
            r_q[hf, me] = s_q[hf, c, z]
            scatter(lambda zz, cc: s_q.at[hf, cc, zz], r_q.at[hf, me], sem_q.at[0, hf], sem_q.at[1, hf])

    def whole(n, k):
        landed(r_p.at[n], sem_p.at[0, n], sem_p.at[1, n]).wait_recv()
        fp[k * block:(k + 1) * block, :] = r_p[n].astype(F32).reshape(block, cols)

    def part(hf):
        landed(r_q.at[hf], sem_q.at[0, hf], sem_q.at[1, hf]).wait_recv()
        view = fp.reshape(ch, rows, cols)
        view[devs:, hf * hr:(hf + 1) * hr, :] = r_q[hf].astype(F32)

    def updated(u, r):
        sl = pl.ds(pl.multiple_of(r * cols, cols), cols)
        mixed = norm_sublanes(fp[pl.ds(r, ch, stride=rows), :], mgt[u]).astype(BF16)
        upd = dot(mixed, mo_ref[u], TN)
        src = x_ref if u == 0 else zb
        zb[sl, :] = (src[sl, :].astype(F32) + gate[sl, :] * upd).astype(BF16)

    def rows_loop(f, lo=0, hi=rows, step=2):
        def some(i, carry):
            for t in range(step):
                f(lo + i * step + t)
            return carry

        lax.fori_loop(0, (hi - lo) // step, some, 0)

    def first_row(r):
        project(0, r)

    rows_loop(first_row)
    pl.semaphore_wait(barrier, (2 * reach) * nc + 1)
    tell(reach, 0)
    pack(0)
    send_first(0, 1, reach)
    pack(1)
    send_first(1, 1, reach)
    for load in loads[4:]:
        load.wait()
    by_channel(1)
    hear(0)
    tell(2 * reach, 1)
    send_first(0, reach + 1, 2 * reach)
    send_first(1, reach + 1, 2 * reach)
    rows_loop(functools.partial(gate_row, 0))
    hear(1)
    send_first(0, 2 * reach + 1, half)
    send_first(1, 2 * reach + 1, half)
    for w in range(2):
        mgt[w] = jnp.transpose(jnp.broadcast_to(mg_ref[w:w + 1, :], (ch, ch)))
    for q in range(4):
        apt[q * ch:(q + 1) * ch, :] = jnp.transpose(
            ap_ref[:, q * ch:(q + 1) * ch].astype(F32)).astype(BF16)
    for k in range(per):
        product(0, k)
    whole(0, 0)
    for hf in range(2):
        part(hf)

        def both_steps(r, hf=hf):
            updated(0, r)
            project(1, r, hf)

        rows_loop(both_steps, hf * hr, (hf + 1) * hr)
        for k in range(per):
            send_second(hf, k)
    rows_loop(functools.partial(gate_row, 1))
    for k in range(per):
        product(1, k)

    def normed_row(r):
        sl = pl.ds(pl.multiple_of(r * cols, cols), cols)
        normed = norm_lanes(zb[sl, :].astype(F32), ag_ref[...]).astype(BF16)
        nall[c, sl, :] = normed
        fb[pl.ds(r, HEADS, stride=rows), :] = dot(ab_ref[...], normed, NT)

    whole(1, 0)
    whole(2, 1)

    def last_steps(r):
        updated(1, r)
        normed_row(r)

    rows_loop(last_steps, step=4)
    s_b[...] = fb[...].astype(BF16)
    to = z // half
    lots = half // stride
    many = nc * lots
    res = lax.rem(z, stride)
    turn = lax.rem(z, half) // stride
    slot = res * many + turn * nc + c
    hops = nz // stride

    def bias_wait(count, ssem, rsem):
        return remote(r_b.at[pl.ds(0, count)], r_b.at[pl.ds(0, count)], ssem, rsem, z, other)

    for t in sorted(range(1, hops), key=lambda t: -min(t, hops - t)):
        remote(s_b, r_b.at[slot], sem_b.at[0], sem_bf.at[turn], lax.rem(z + stride * t, nz), to).start()

    @pl.when(to == c)
    def _():
        r_b[slot] = s_b[...]

    @pl.when(to != c)
    def _():
        remote(s_b, r_b.at[slot], sem_b.at[0], sem_bf.at[turn], z, other).start()

    swap = remote(nall.at[c], nall.at[c], sem_n.at[0], sem_n.at[1], z, other)
    swap.start()

    def scores_row(r):
        sl = pl.ds(pl.multiple_of(r * cols, cols), cols)
        mine_n = nall[c, sl, :]
        full = jnp.concatenate([nall[cc, sl, :] for cc in range(nc)], axis=0)
        qt = dot(apt[:ch], mine_n, NT).astype(BF16)
        gt = dot(apt[3 * ch:], mine_n, NT).astype(BF16)
        keys = dot(full, ap_ref[:, ch:2 * ch], NN).astype(BF16)
        vt[r] = dot(apt[2 * ch:3 * ch], full, NT).astype(BF16)
        sg[r] = jax.nn.sigmoid(gt.astype(F32))
        wide = []
        for h in range(HEADS):
            parts = [jnp.zeros((h * hd, cols), BF16)] if h else []
            parts.append(qt[h * hd:(h + 1) * hd])
            if h < HEADS - 1:
                parts.append(jnp.zeros(((HEADS - 1 - h) * hd, cols), BF16))
            wide.append(jnp.concatenate(parts, axis=0))
        sc[r] = dot(keys, jnp.concatenate(wide, axis=1), NN) * (1.0 / float(hd) ** 0.5)

    swap.wait()
    rows_loop(scores_row)

    ahead = lax.rem(z + nz - c * half, nz)
    rising = (ahead < half // 2) | (ahead >= nz - half // 2)
    order = [jnp.where(rising, i, lots - 1 - i) for i in range(lots)]
    near = [lax.rem(z + nz + o, nz) for o in (2, 1, -1)]
    for m in order:
        here = c * half + m * stride + res == z

        @pl.when(here)
        def _(m=m):
            bias_wait(nc - 1, sem_b.at[0], sem_bf.at[m]).wait_recv()

        @pl.when(jnp.logical_not(here))
        def _(m=m):
            bias_wait(nc, sem_b.at[0], sem_bf.at[m]).wait_recv()

        group = r_b.at[pl.ds(res * many + m * nc, nc)]
        for beside in near:
            remote(group, group, sem_b.at[1], sem_bs.at[m], beside, c).start()

    for m in order:
        bias_wait(len(near) * nc, sem_b.at[1], sem_bs.at[m]).wait_recv()
    for kc in range(nc):
        part = [
            jnp.stack([r_b[q * many + m * nc + kc] for m in range(lots)]).astype(F32) for q in range(stride)
        ]
        for h in range(HEADS):
            tile = jnp.stack([p[:, h * rows:(h + 1) * rows] for p in part], axis=1).reshape(half * rows, cols)
            tile = tile + km_ref[:, kc * cols:(kc + 1) * cols]
            bt[kc * cols:(kc + 1) * cols, h * cols:(h + 1) * cols] = jnp.transpose(tile)

    def attend_row(r):
        sl = pl.ds(pl.multiple_of(r * cols, cols), cols)
        score = sc[r] + bt[...]
        top = jnp.max(score, axis=0, keepdims=True)
        e = jnp.exp(score - top)
        inv = 1.0 / jnp.sum(e, axis=0, keepdims=True)
        got = dot(vt[r], e.astype(BF16), NN)
        parts = []
        for h in range(HEADS):
            lanes = slice(h * cols, (h + 1) * cols)
            parts.append(got[h * hd:(h + 1) * hd, lanes] * inv[:, lanes])
        gated = (sg[r] * jnp.concatenate(parts, axis=0)).astype(BF16)
        ob[r] = (zb[sl, :].astype(F32) + dot(gated, ao_ref[...], TN)).astype(BF16)

    def leave(i):
        some = pl.ds(i * 2, 2)
        return pltpu.make_async_copy(ob.at[some], out_hbm.at[some], sem_o.at[i])

    def two_rows(i, carry):
        attend_row(2 * i)
        attend_row(2 * i + 1)
        leave(i).start()
        return carry

    lax.fori_loop(0, rows // 2, two_rows, 0)

    for k in range(per):
        landed(r_lr.at[k], sem_lr.at[0, k], sem_lr.at[1, k]).wait_send()
        landed(r_q.at[k], sem_q.at[0, k], sem_q.at[1, k]).wait_send()
        for hf in range(2):
            landed(r_l2.at[hf, k], sem_l2.at[0, hf, k], sem_l2.at[1, hf, k]).wait_send()
    for n in range(3):
        landed(r_p.at[n], sem_p.at[0, n], sem_p.at[1, n]).wait_send()

    @pl.when(to == c)
    def _():
        bias_wait(hops - 1, sem_b.at[0], sem_bf.at[0]).wait_send()

    @pl.when(to != c)
    def _():
        bias_wait(hops, sem_b.at[0], sem_bf.at[0]).wait_send()

    bias_wait(len(near) * many, sem_b.at[1], sem_bf.at[0]).wait_send()
    for i in range(rows // 2):
        leave(i).wait()


def solution(mesh):
    nz, nc = mesh.shape["row"], mesh.shape["col"]
    devs = nz * nc

    def local(pair_rep, residue_mask, crop_length, norm_gain, mult_proj, mixed_gain, mult_out, att_gain, att_proj,
              att_bias, att_out):
        rows, cols, ch = pair_rep.shape
        per = ch // devs
        half = nz // 2
        stride = 4
        lots = half // stride
        area = rows * cols
        vmem = pltpu.VMEM
        out = pl.pallas_call(
            functools.partial(kernel, nz, nc, rows, stride, 4),
            out_shape=jax.ShapeDtypeStruct((rows, cols, ch), BF16),
            in_specs=[pl.BlockSpec(memory_space=pltpu.SMEM)] + [pl.BlockSpec(memory_space=pl.ANY)] * 10,
            out_specs=pl.BlockSpec(memory_space=pl.ANY),
            scratch_shapes=[
                vmem((1, nc * cols), jnp.int32),
                vmem((area, ch), BF16),
                vmem(norm_gain.shape, F32),
                vmem(mult_proj.shape, BF16),
                vmem(mixed_gain.shape, F32),
                vmem(mult_out.shape, BF16),
                vmem((1, ch), F32),
                vmem(att_proj.shape, BF16),
                vmem((HEADS, ch), BF16),
                vmem(att_out.shape, BF16),
                pltpu.SemaphoreType.DMA((10,)),
                vmem((rows, cols), F32),
                vmem((1, nc * cols), F32),
                vmem((2, 4 * ch, ch), BF16),
                vmem((2, ch, ch), F32),
                vmem((4 * ch, ch), BF16),
                vmem((area, ch), BF16),
                vmem((area, ch), F32),
                vmem((area, ch), BF16),
                vmem((ch * rows, cols), F32),
                vmem((ch * rows, cols), F32),
                vmem((ch * rows, cols), F32),
                vmem((per, devs, 2 * rows, cols), BF16),
                vmem((per, devs, 2 * rows, cols), BF16),
                vmem((2, per, devs, rows, cols), BF16),
                vmem((2, per, devs, rows, cols), BF16),
                vmem((3, nc, nz, rows, cols), BF16),
                vmem((3, devs, rows, cols), BF16),
                vmem((2, nc, nz, rows // 2, cols), BF16),
                vmem((2, devs, rows // 2, cols), BF16),
                vmem((nc, area, ch), BF16),
                vmem((HEADS * rows, cols), F32),
                vmem((HEADS * rows, cols), BF16),
                vmem((nc * half, HEADS * rows, cols), BF16),
                vmem((nc * cols, HEADS * cols), F32),
                vmem((rows, nc * cols, HEADS * cols), F32),
                vmem((rows, ch, nc * cols), BF16),
                vmem((rows, ch, cols), F32),
                vmem((rows, cols, ch), BF16),
                pltpu.SemaphoreType.REGULAR((2, 2)),
                pltpu.SemaphoreType.DMA((2, per)),
                pltpu.SemaphoreType.DMA((2, 2, per)),
                pltpu.SemaphoreType.DMA((2, 3)),
                pltpu.SemaphoreType.DMA((2, 2)),
                pltpu.SemaphoreType.DMA((2,)),
                pltpu.SemaphoreType.DMA((lots,)),
                pltpu.SemaphoreType.DMA((lots,)),
                pltpu.SemaphoreType.DMA((2,)),
                pltpu.SemaphoreType.DMA((rows // 2,)),
            ],
            compiler_params=pltpu.CompilerParams(
                collective_id=1, has_side_effects=True, vmem_limit_bytes=62 * 1024 * 1024
            ),
            name="triangle",
        )(
            crop_length, residue_mask.reshape(1, nc * cols), pair_rep.reshape(area, ch), norm_gain, mult_proj,
            mixed_gain, mult_out, att_gain.reshape(1, ch), att_proj, att_bias.T, att_out,
        )
        return out

    return jax.shard_map(
        local,
        mesh=mesh,
        in_specs=(P(("groups", "row"), "col", None), P("groups"), P("groups")) + (P(),) * 8,
        out_specs=P(("groups", "row"), "col", None),
        check_vma=False,
    )
```

```python
import functools

import jax
import jax.numpy as jnp
from jax import lax
from jax.experimental import pallas as pl
from jax.experimental.pallas import tpu as pltpu
from jax.sharding import PartitionSpec as P

HEADS = 4
EPSILON = 1e-05
LOG2E = 1.4426950408889634
MESH = pl.DeviceIdType.MESH
F32 = jnp.float32
BF16 = jnp.bfloat16
NN = (((1,), (0,)), ((), ()))
NT = (((1,), (1,)), ((), ()))
TN = (((0,), (0,)), ((), ()))


def dot(a, b, dims):
    return lax.dot_general(a, b, dims, preferred_element_type=F32)


def norm_lanes(v, gain):
    mean = jnp.mean(v, axis=-1, keepdims=True)
    cen = v - mean
    var = jnp.mean(cen * cen, axis=-1, keepdims=True)
    return cen * lax.rsqrt(var + EPSILON) * gain


def norm_sublanes(v, gain):
    mean = jnp.mean(v, axis=0, keepdims=True)
    cen = v - mean
    var = jnp.mean(cen * cen, axis=0, keepdims=True)
    return cen * lax.rsqrt(var + EPSILON) * gain


def kernel(
    nz, nc, rows, stride, reach, crop_ref, rm_hbm, x_hbm, ng_hbm, mp_hbm, mg_hbm, mo_hbm, ag_hbm, ap_hbm, ab_hbm, ao_hbm,
    out_hbm,
    rm_ref, x_ref, ng_ref, mp_ref, mg_ref, mo_ref, ag_ref, ap_ref, ab_ref, ao_ref, sem_in,
    pm_ref, km_ref, wt, mgt, apt, nrm, gate, zb, fl, fr, fp, s_lr, r_lr, s_l2, r_l2, s_p, r_p, s_q, r_q, nall, fb, s_b, r_b, bt, sc, vt, sg, ob,
    level, sem_lr, sem_l2, sem_p, sem_q, sem_n, sem_bf, sem_bs, sem_b, sem_o,
):
    z = lax.axis_index("row")
    c = lax.axis_index("col")
    me = z * nc + c
    devs = nz * nc
    cols = pm_ref.shape[1]
    ch = x_ref.shape[1]
    hd = ch // HEADS
    per = s_lr.shape[0]
    block = devs * rows
    half = nz // 2
    other = 1 - c

    barrier = pltpu.get_barrier_semaphore()

    for d in range(1, reach + 1):
        for zz in (lax.rem(z + d, nz), lax.rem(z + nz - d, nz)):
            for cc in (c, other):
                pl.semaphore_signal(barrier, inc=1, device_id={"row": zz, "col": cc}, device_id_type=MESH)
    pl.semaphore_signal(barrier, inc=1, device_id={"row": z, "col": other}, device_id_type=MESH)
    loads = []
    for i, (src, dst) in enumerate((
        (x_hbm, x_ref), (ng_hbm, ng_ref), (mp_hbm, mp_ref), (rm_hbm, rm_ref), (mg_hbm, mg_ref), (mo_hbm, mo_ref),
        (ag_hbm, ag_ref), (ap_hbm, ap_ref), (ab_hbm, ab_ref), (ao_hbm, ao_ref),
    )):
        loads.append(pltpu.make_async_copy(src, dst, sem_in.at[i]))
        loads[-1].start()

    def tell(d, n):
        up, down = lax.rem(z + d, nz), lax.rem(z + nz - d, nz)
        pl.semaphore_signal(level.at[0, n], inc=1, device_id={"row": up, "col": c}, device_id_type=MESH)
        pl.semaphore_signal(level.at[1, n], inc=1, device_id={"row": down, "col": c}, device_id_type=MESH)

    def hear(n):
        pl.semaphore_wait(level.at[0, n], 1)
        pl.semaphore_wait(level.at[1, n], 1)

    def remote(src, dst, ssem, rsem, zz, cc):
        return pltpu.make_async_remote_copy(
            src_ref=src, dst_ref=dst, send_sem=ssem, recv_sem=rsem,
            device_id={"row": zz, "col": cc}, device_id_type=MESH,
        )

    def ring(src_at, dst, ssem, rsem, near, far):
        def put(zz):
            remote(src_at(zz, c), dst, ssem, rsem, zz, c).start()
            remote(src_at(zz, other), dst, ssem, rsem, zz, other).start()

        def both(i, carry):
            up, down = z + far - i, z - far + i
            put(jnp.where(up >= nz, up - nz, up))
            put(jnp.where(down < 0, down + nz, down))
            return carry

        if far == half:
            put(lax.rem(z + half, nz))
            far -= 1
        lax.fori_loop(0, far + 1 - near, both, 0)
        if near == 1:
            remote(src_at(z, other), dst, ssem, rsem, z, other).start()

    def scatter(src_at, dst, ssem, rsem):
        ring(src_at, dst, ssem, rsem, 1, half)

    def landed(buf, ssem, rsem):
        every = buf.at[pl.ds(0, devs - 1)]
        return remote(every, every, ssem, rsem, z, other)

    for load in loads[:4]:
        load.wait()
    pos = lax.broadcasted_iota(jnp.int32, rm_ref.shape, 1)
    alive = jnp.where(((rm_ref[...] == 1) | (pos == 0)) & (pos < crop_ref[0]), 1.0, 0.0).astype(F32)
    km_ref[...] = jnp.where(alive > 0.0, 0.0, -1000000000.0).astype(F32)
    spot = lax.broadcasted_iota(jnp.int32, (rows, nc * cols), 1)
    want = lax.broadcasted_iota(jnp.int32, (rows, nc * cols), 0) + z * rows
    row_alive = jnp.sum(jnp.where(spot == want, alive, 0.0), axis=1, keepdims=True)
    col_alive = alive[:, :cols]
    for cc in range(1, nc):
        col_alive = jnp.where(c == cc, alive[:, cc * cols:(cc + 1) * cols], col_alive)
    pm_ref[...] = row_alive * col_alive

    def by_channel(u):
        for q in range(4):
            wt[u, q * ch:(q + 1) * ch, :] = jnp.transpose(
                mp_ref[u, :, q * ch:(q + 1) * ch].astype(F32)).astype(BF16)

    by_channel(0)

    hr = rows // 2

    def project(u, r, hf=0):
        sl = pl.ds(pl.multiple_of(r * cols, cols), cols)
        src = x_ref if u == 0 else zb
        normed = norm_lanes(src[sl, :].astype(F32), ng_ref[u:u + 1, :]).astype(BF16)
        nrm[sl, :] = normed
        pt = dot(wt[u], normed, NT)
        mask = pm_ref[pl.ds(r, 1), :]
        left = mask * jax.nn.sigmoid(pt[ch:2 * ch]) * pt[:ch]
        right = mask * jax.nn.sigmoid(pt[3 * ch:]) * pt[2 * ch:3 * ch]
        if u == 0:
            fl[pl.ds(r, ch, stride=rows), :] = left
            fr[pl.ds(r, ch, stride=rows), :] = right
        elif hf == 0:
            fl[pl.ds(r, ch, stride=rows), :] = left
            fl[pl.ds(r + hr, ch, stride=rows), :] = right
        else:
            fr[pl.ds(r, ch, stride=rows), :] = left
            fr[pl.ds(r - hr, ch, stride=rows), :] = right

    def pack(k):
        pair = jnp.concatenate(
            [
                fl[k * block:(k + 1) * block, :].reshape(devs, rows, cols),
                fr[k * block:(k + 1) * block, :].reshape(devs, rows, cols),
            ],
            axis=1,
        )
        s_lr[k] = pair.astype(BF16)
        r_lr[k, c * nz + z] = s_lr[k, me]

    def send_first(k, near, far):
        ring(lambda zz, cc: s_lr.at[k, zz * nc + cc], r_lr.at[k, c * nz + z], sem_lr.at[0, k], sem_lr.at[1, k], near, far)

    def send_second(hf, k):
        src = fl if hf == 0 else fr
        s_l2[hf, k] = src[k * block:(k + 1) * block, :].reshape(devs, rows, cols).astype(BF16)
        r_l2[hf, k, c * nz + z] = s_l2[hf, k, me]
        scatter(
            lambda zz, cc: s_l2.at[hf, k, zz * nc + cc], r_l2.at[hf, k, c * nz + z],
            sem_l2.at[0, hf, k], sem_l2.at[1, hf, k])

    def gate_row(u, r):
        sl = pl.ds(pl.multiple_of(r * cols, cols), cols)
        gate[sl, :] = jax.nn.sigmoid(dot(nrm[sl, :], mp_ref[u, :, 4 * ch:], NN))

    def product(u, k):
        lefts, rights = [], []
        if u == 0:
            landed(r_lr.at[k], sem_lr.at[0, k], sem_lr.at[1, k]).wait_recv()
            for cc in range(nc):
                part = r_lr[k, cc * nz:(cc + 1) * nz].astype(F32)
                lefts.append(part[:, :rows].reshape(nz * rows, cols).astype(BF16))
                rights.append(part[:, rows:].reshape(nz * rows, cols).astype(BF16))
        else:
            for hf in range(2):
                landed(r_l2.at[hf, k], sem_l2.at[0, hf, k], sem_l2.at[1, hf, k]).wait_recv()
            low = lax.broadcasted_iota(jnp.int32, (nz, rows, cols), 1) < hr
            for cc in range(nc):
                first = r_l2[0, k, cc * nz:(cc + 1) * nz].astype(F32)
                last = r_l2[1, k, cc * nz:(cc + 1) * nz].astype(F32)
                lefts.append(jnp.where(low, first, last).reshape(nz * rows, cols).astype(BF16))
                turned = pltpu.roll(jnp.where(low, last, first), hr, 1)
                rights.append(turned.reshape(nz * rows, cols).astype(BF16))
        left = jnp.concatenate(lefts, axis=1)
        right = jnp.concatenate(rights, axis=1)
        prod = dot(left, right, NT if u == 0 else TN)
        tiles = [prod[:, cc * cols:(cc + 1) * cols].reshape(nz, rows, cols) for cc in range(nc)]
        if u or k == 0:
            n = u + k
            for cc in range(nc):
                s_p[n, cc] = tiles[cc].astype(BF16)
            r_p[n, me] = s_p[n, c, z]
            scatter(lambda zz, cc: s_p.at[n, cc, zz], r_p.at[n, me], sem_p.at[0, n], sem_p.at[1, n])
            return
        for hf in range(2):
            for cc in range(nc):
                s_q[hf, cc] = tiles[cc][:, hf * hr:(hf + 1) * hr].astype(BF16)
            r_q[hf, me] = s_q[hf, c, z]
            scatter(lambda zz, cc: s_q.at[hf, cc, zz], r_q.at[hf, me], sem_q.at[0, hf], sem_q.at[1, hf])

    def whole(n, k):
        landed(r_p.at[n], sem_p.at[0, n], sem_p.at[1, n]).wait_recv()
        fp[k * block:(k + 1) * block, :] = r_p[n].astype(F32).reshape(block, cols)

    def part(hf):
        landed(r_q.at[hf], sem_q.at[0, hf], sem_q.at[1, hf]).wait_recv()
        view = fp.reshape(ch, rows, cols)
        view[devs:, hf * hr:(hf + 1) * hr, :] = r_q[hf].astype(F32)

    def updated(u, r):
        sl = pl.ds(pl.multiple_of(r * cols, cols), cols)
        mixed = norm_sublanes(fp[pl.ds(r, ch, stride=rows), :], mgt[u]).astype(BF16)
        upd = dot(mixed, mo_ref[u], TN)
        src = x_ref if u == 0 else zb
        zb[sl, :] = (src[sl, :].astype(F32) + gate[sl, :] * upd).astype(BF16)

    def rows_loop(f, lo=0, hi=rows, step=2):
        def some(i, carry):
            for t in range(step):
                f(lo + i * step + t)
            return carry

        lax.fori_loop(0, (hi - lo) // step, some, 0)

    def first_row(r):
        project(0, r)

    rows_loop(first_row, step=4)
    pl.semaphore_wait(barrier, (2 * reach) * nc + 1)
    tell(reach, 0)
    pack(0)
    send_first(0, 1, reach)
    pack(1)
    send_first(1, 1, reach)
    for load in loads[4:]:
        load.wait()
    by_channel(1)
    hear(0)
    tell(2 * reach, 1)
    send_first(0, reach + 1, 2 * reach)
    send_first(1, reach + 1, 2 * reach)
    rows_loop(functools.partial(gate_row, 0))
    hear(1)
    send_first(0, 2 * reach + 1, half)
    send_first(1, 2 * reach + 1, half)
    for w in range(2):
        mgt[w] = jnp.transpose(jnp.broadcast_to(mg_ref[w:w + 1, :], (ch, ch)))
    for q in range(4):
        apt[q * ch:(q + 1) * ch, :] = jnp.transpose(
            ap_ref[:, q * ch:(q + 1) * ch].astype(F32)).astype(BF16)
    for k in range(per):
        product(0, k)
    whole(0, 0)
    for hf in range(2):
        part(hf)

        def both_steps(r, hf=hf):
            updated(0, r)
            project(1, r, hf)

        rows_loop(both_steps, hf * hr, (hf + 1) * hr, step=4)
        for k in range(per):
            send_second(hf, k)
    rows_loop(functools.partial(gate_row, 1))
    for k in range(per):
        product(1, k)

    def normed_row(r):
        sl = pl.ds(pl.multiple_of(r * cols, cols), cols)
        normed = norm_lanes(zb[sl, :].astype(F32), ag_ref[...]).astype(BF16)
        nall[c, sl, :] = normed
        fb[pl.ds(r, HEADS, stride=rows), :] = dot(ab_ref[...], normed, NT)

    whole(1, 0)
    whole(2, 1)

    def last_steps(r):
        updated(1, r)
        normed_row(r)

    rows_loop(last_steps, step=4)
    s_b[...] = fb[...].astype(BF16)
    to = z // half
    lots = half // stride
    many = nc * lots
    res = lax.rem(z, stride)
    turn = lax.rem(z, half) // stride
    slot = res * many + turn * nc + c
    hops = nz // stride

    def bias_wait(count, ssem, rsem):
        return remote(r_b.at[pl.ds(0, count)], r_b.at[pl.ds(0, count)], ssem, rsem, z, other)

    for t in sorted(range(1, hops), key=lambda t: -min(t, hops - t)):
        remote(s_b, r_b.at[slot], sem_b.at[0], sem_bf.at[turn], lax.rem(z + stride * t, nz), to).start()

    @pl.when(to == c)
    def _():
        r_b[slot] = s_b[...]

    @pl.when(to != c)
    def _():
        remote(s_b, r_b.at[slot], sem_b.at[0], sem_bf.at[turn], z, other).start()

    swap = remote(nall.at[c], nall.at[c], sem_n.at[0], sem_n.at[1], z, other)
    swap.start()

    def scores_row(r):
        sl = pl.ds(pl.multiple_of(r * cols, cols), cols)
        mine_n = nall[c, sl, :]
        full = jnp.concatenate([nall[cc, sl, :] for cc in range(nc)], axis=0)
        qt = dot(apt[:ch], mine_n, NT).astype(BF16)
        gt = dot(apt[3 * ch:], mine_n, NT).astype(BF16)
        keys = dot(full, ap_ref[:, ch:2 * ch], NN).astype(BF16)
        vt[r] = dot(apt[2 * ch:3 * ch], full, NT).astype(BF16)
        sg[r] = jax.nn.sigmoid(gt.astype(F32))
        wide = []
        for h in range(HEADS):
            parts = [jnp.zeros((h * hd, cols), BF16)] if h else []
            parts.append(qt[h * hd:(h + 1) * hd])
            if h < HEADS - 1:
                parts.append(jnp.zeros(((HEADS - 1 - h) * hd, cols), BF16))
            wide.append(jnp.concatenate(parts, axis=0))
        sc[r] = dot(keys, jnp.concatenate(wide, axis=1), NN) * (LOG2E / float(hd) ** 0.5)

    swap.wait()
    rows_loop(scores_row)

    ahead = lax.rem(z + nz - c * half, nz)
    rising = (ahead < half // 2) | (ahead >= nz - half // 2)
    order = [jnp.where(rising, i, lots - 1 - i) for i in range(lots)]
    near = [lax.rem(z + nz + o, nz) for o in (2, 1, -1)]
    for m in order:
        here = c * half + m * stride + res == z

        @pl.when(here)
        def _(m=m):
            bias_wait(nc - 1, sem_b.at[0], sem_bf.at[m]).wait_recv()

        @pl.when(jnp.logical_not(here))
        def _(m=m):
            bias_wait(nc, sem_b.at[0], sem_bf.at[m]).wait_recv()

        group = r_b.at[pl.ds(res * many + m * nc, nc)]
        for beside in near:
            remote(group, group, sem_b.at[1], sem_bs.at[m], beside, c).start()

    for m in order:
        bias_wait(len(near) * nc, sem_b.at[1], sem_bs.at[m]).wait_recv()
    for kc in range(nc):
        part = [
            jnp.stack([r_b[q * many + m * nc + kc] for m in range(lots)]).astype(F32) for q in range(stride)
        ]
        for h in range(HEADS):
            tile = jnp.stack([p[:, h * rows:(h + 1) * rows] for p in part], axis=1).reshape(half * rows, cols)
            tile = tile + km_ref[:, kc * cols:(kc + 1) * cols]
            bt[kc * cols:(kc + 1) * cols, h * cols:(h + 1) * cols] = jnp.transpose(tile * LOG2E)

    def attend_row(r):
        sl = pl.ds(pl.multiple_of(r * cols, cols), cols)
        score = sc[r] + bt[...]
        top = jnp.max(score, axis=0, keepdims=True)
        e = jnp.exp2(score - top)
        inv = 1.0 / jnp.sum(e, axis=0, keepdims=True)
        got = dot(vt[r], e.astype(BF16), NN)
        parts = []
        for h in range(HEADS):
            lanes = slice(h * cols, (h + 1) * cols)
            parts.append(got[h * hd:(h + 1) * hd, lanes] * inv[:, lanes])
        gated = (sg[r] * jnp.concatenate(parts, axis=0)).astype(BF16)
        ob[r] = (zb[sl, :].astype(F32) + dot(gated, ao_ref[...], TN)).astype(BF16)

    at_once = 4

    def leave(i):
        some = pl.ds(i * at_once, at_once)
        return pltpu.make_async_copy(ob.at[some], out_hbm.at[some], sem_o.at[i])

    def some_rows(i, carry):
        for t in range(at_once):
            attend_row(at_once * i + t)
        leave(i).start()
        return carry

    lax.fori_loop(0, rows // at_once, some_rows, 0)

    for k in range(per):
        landed(r_lr.at[k], sem_lr.at[0, k], sem_lr.at[1, k]).wait_send()
        landed(r_q.at[k], sem_q.at[0, k], sem_q.at[1, k]).wait_send()
        for hf in range(2):
            landed(r_l2.at[hf, k], sem_l2.at[0, hf, k], sem_l2.at[1, hf, k]).wait_send()
    for n in range(3):
        landed(r_p.at[n], sem_p.at[0, n], sem_p.at[1, n]).wait_send()

    @pl.when(to == c)
    def _():
        bias_wait(hops - 1, sem_b.at[0], sem_bf.at[0]).wait_send()

    @pl.when(to != c)
    def _():
        bias_wait(hops, sem_b.at[0], sem_bf.at[0]).wait_send()

    bias_wait(len(near) * many, sem_b.at[1], sem_bf.at[0]).wait_send()
    for i in range(rows // at_once):
        leave(i).wait()


def solution(mesh):
    nz, nc = mesh.shape["row"], mesh.shape["col"]
    devs = nz * nc

    def local(pair_rep, residue_mask, crop_length, norm_gain, mult_proj, mixed_gain, mult_out, att_gain, att_proj,
              att_bias, att_out):
        rows, cols, ch = pair_rep.shape
        per = ch // devs
        half = nz // 2
        stride = 4
        lots = half // stride
        area = rows * cols
        vmem = pltpu.VMEM
        out = pl.pallas_call(
            functools.partial(kernel, nz, nc, rows, stride, 4),
            out_shape=jax.ShapeDtypeStruct((rows, cols, ch), BF16),
            in_specs=[pl.BlockSpec(memory_space=pltpu.SMEM)] + [pl.BlockSpec(memory_space=pl.ANY)] * 10,
            out_specs=pl.BlockSpec(memory_space=pl.ANY),
            scratch_shapes=[
                vmem((1, nc * cols), jnp.int32),
                vmem((area, ch), BF16),
                vmem(norm_gain.shape, F32),
                vmem(mult_proj.shape, BF16),
                vmem(mixed_gain.shape, F32),
                vmem(mult_out.shape, BF16),
                vmem((1, ch), F32),
                vmem(att_proj.shape, BF16),
                vmem((HEADS, ch), BF16),
                vmem(att_out.shape, BF16),
                pltpu.SemaphoreType.DMA((10,)),
                vmem((rows, cols), F32),
                vmem((1, nc * cols), F32),
                vmem((2, 4 * ch, ch), BF16),
                vmem((2, ch, ch), F32),
                vmem((4 * ch, ch), BF16),
                vmem((area, ch), BF16),
                vmem((area, ch), F32),
                vmem((area, ch), BF16),
                vmem((ch * rows, cols), F32),
                vmem((ch * rows, cols), F32),
                vmem((ch * rows, cols), F32),
                vmem((per, devs, 2 * rows, cols), BF16),
                vmem((per, devs, 2 * rows, cols), BF16),
                vmem((2, per, devs, rows, cols), BF16),
                vmem((2, per, devs, rows, cols), BF16),
                vmem((3, nc, nz, rows, cols), BF16),
                vmem((3, devs, rows, cols), BF16),
                vmem((2, nc, nz, rows // 2, cols), BF16),
                vmem((2, devs, rows // 2, cols), BF16),
                vmem((nc, area, ch), BF16),
                vmem((HEADS * rows, cols), F32),
                vmem((HEADS * rows, cols), BF16),
                vmem((nc * half, HEADS * rows, cols), BF16),
                vmem((nc * cols, HEADS * cols), F32),
                vmem((rows, nc * cols, HEADS * cols), F32),
                vmem((rows, ch, nc * cols), BF16),
                vmem((rows, ch, cols), F32),
                vmem((rows, cols, ch), BF16),
                pltpu.SemaphoreType.REGULAR((2, 2)),
                pltpu.SemaphoreType.DMA((2, per)),
                pltpu.SemaphoreType.DMA((2, 2, per)),
                pltpu.SemaphoreType.DMA((2, 3)),
                pltpu.SemaphoreType.DMA((2, 2)),
                pltpu.SemaphoreType.DMA((2,)),
                pltpu.SemaphoreType.DMA((lots,)),
                pltpu.SemaphoreType.DMA((lots,)),
                pltpu.SemaphoreType.DMA((2,)),
                pltpu.SemaphoreType.DMA((rows // 2,)),
            ],
            compiler_params=pltpu.CompilerParams(
                collective_id=1, has_side_effects=True, vmem_limit_bytes=62 * 1024 * 1024
            ),
            name="triangle",
        )(
            crop_length, residue_mask.reshape(1, nc * cols), pair_rep.reshape(area, ch), norm_gain, mult_proj,
            mixed_gain, mult_out, att_gain.reshape(1, ch), att_proj, att_bias.T, att_out,
        )
        return out

    return jax.shard_map(
        local,
        mesh=mesh,
        in_specs=(P(("groups", "row"), "col", None), P("groups"), P("groups")) + (P(),) * 8,
        out_specs=P(("groups", "row"), "col", None),
        check_vma=False,
    )
```

```python
import functools

import jax
import jax.numpy as jnp
from jax import lax
from jax.experimental import pallas as pl
from jax.experimental.pallas import tpu as pltpu
from jax.sharding import PartitionSpec as P

HEADS = 4
EPSILON = 1e-05
LOG2E = 1.4426950408889634
MESH = pl.DeviceIdType.MESH
F32 = jnp.float32
BF16 = jnp.bfloat16
NN = (((1,), (0,)), ((), ()))
NT = (((1,), (1,)), ((), ()))
TN = (((0,), (0,)), ((), ()))


def dot(a, b, dims):
    return lax.dot_general(a, b, dims, preferred_element_type=F32)


def norm_lanes(v, gain):
    mean = jnp.mean(v, axis=-1, keepdims=True)
    cen = v - mean
    var = jnp.mean(cen * cen, axis=-1, keepdims=True)
    return cen * lax.rsqrt(var + EPSILON) * gain


def norm_sublanes(v, gain):
    mean = jnp.mean(v, axis=0, keepdims=True)
    cen = v - mean
    var = jnp.mean(cen * cen, axis=0, keepdims=True)
    return cen * lax.rsqrt(var + EPSILON) * gain


def kernel(
    nz, nc, rows, stride, reach, crop_ref, rm_hbm, x_hbm, ng_hbm, mp_hbm, mg_hbm, mo_hbm, ag_hbm, ap_hbm, ab_hbm, ao_hbm,
    out_hbm,
    rm_ref, x_ref, ng_ref, mp_ref, mg_ref, mo_ref, ag_ref, ap_ref, ab_ref, ao_ref, sem_in,
    pm_ref, km_ref, wt, mgt, apt, nrm, gate, zb, fl, fr, fp, s_lr, r_lr, s_l2, r_l2, s_p, r_p, s_q, r_q, nall, fb, s_b, r_b, bt, sc, vt, sg, ob,
    level, sem_lr, sem_l2, sem_p, sem_q, sem_n, sem_bf, sem_bs, sem_b, sem_o,
):
    z = lax.axis_index("row")
    c = lax.axis_index("col")
    me = z * nc + c
    devs = nz * nc
    cols = pm_ref.shape[1]
    ch = x_ref.shape[1]
    hd = ch // HEADS
    per = s_lr.shape[0]
    block = devs * rows
    half = nz // 2
    other = 1 - c

    barrier = pltpu.get_barrier_semaphore()

    for d in range(1, reach + 1):
        for zz in (lax.rem(z + d, nz), lax.rem(z + nz - d, nz)):
            for cc in (c, other):
                pl.semaphore_signal(barrier, inc=1, device_id={"row": zz, "col": cc}, device_id_type=MESH)
    pl.semaphore_signal(barrier, inc=1, device_id={"row": z, "col": other}, device_id_type=MESH)
    loads = []
    for i, (src, dst) in enumerate((
        (x_hbm, x_ref), (ng_hbm, ng_ref), (mp_hbm, mp_ref), (rm_hbm, rm_ref), (mg_hbm, mg_ref), (mo_hbm, mo_ref),
        (ag_hbm, ag_ref), (ap_hbm, ap_ref), (ab_hbm, ab_ref), (ao_hbm, ao_ref),
    )):
        loads.append(pltpu.make_async_copy(src, dst, sem_in.at[i]))
        loads[-1].start()

    def tell(d, n):
        up, down = lax.rem(z + d, nz), lax.rem(z + nz - d, nz)
        pl.semaphore_signal(level.at[0, n], inc=1, device_id={"row": up, "col": c}, device_id_type=MESH)
        pl.semaphore_signal(level.at[1, n], inc=1, device_id={"row": down, "col": c}, device_id_type=MESH)

    def hear(n):
        pl.semaphore_wait(level.at[0, n], 1)
        pl.semaphore_wait(level.at[1, n], 1)

    def remote(src, dst, ssem, rsem, zz, cc):
        return pltpu.make_async_remote_copy(
            src_ref=src, dst_ref=dst, send_sem=ssem, recv_sem=rsem,
            device_id={"row": zz, "col": cc}, device_id_type=MESH,
        )

    def ring(src_at, dst, ssem, rsem, near, far):
        def put(zz):
            remote(src_at(zz, c), dst, ssem, rsem, zz, c).start()
            remote(src_at(zz, other), dst, ssem, rsem, zz, other).start()

        def both(i, carry):
            up, down = z + far - i, z - far + i
            put(jnp.where(up >= nz, up - nz, up))
            put(jnp.where(down < 0, down + nz, down))
            return carry

        if far == half:
            put(lax.rem(z + half, nz))
            far -= 1
        lax.fori_loop(0, far + 1 - near, both, 0)
        if near == 1:
            remote(src_at(z, other), dst, ssem, rsem, z, other).start()

    def scatter(src_at, dst, ssem, rsem):
        ring(src_at, dst, ssem, rsem, 1, half)

    def landed(buf, ssem, rsem):
        every = buf.at[pl.ds(0, devs - 1)]
        return remote(every, every, ssem, rsem, z, other)

    for load in loads[:4]:
        load.wait()
    pos = lax.broadcasted_iota(jnp.int32, rm_ref.shape, 1)
    alive = jnp.where(((rm_ref[...] == 1) | (pos == 0)) & (pos < crop_ref[0]), 1.0, 0.0).astype(F32)
    km_ref[...] = jnp.where(alive > 0.0, 0.0, -1000000000.0).astype(F32)
    spot = lax.broadcasted_iota(jnp.int32, (rows, nc * cols), 1)
    want = lax.broadcasted_iota(jnp.int32, (rows, nc * cols), 0) + z * rows
    row_alive = jnp.sum(jnp.where(spot == want, alive, 0.0), axis=1, keepdims=True)
    col_alive = alive[:, :cols]
    for cc in range(1, nc):
        col_alive = jnp.where(c == cc, alive[:, cc * cols:(cc + 1) * cols], col_alive)
    pm_ref[...] = row_alive * col_alive

    def by_channel(u):
        for q in range(4):
            wt[u, q * ch:(q + 1) * ch, :] = jnp.transpose(
                mp_ref[u, :, q * ch:(q + 1) * ch].astype(F32)).astype(BF16)

    by_channel(0)

    hr = rows // 2

    def project(u, r, hf=0):
        sl = pl.ds(pl.multiple_of(r * cols, cols), cols)
        src = x_ref if u == 0 else zb
        normed = norm_lanes(src[sl, :].astype(F32), ng_ref[u:u + 1, :]).astype(BF16)
        nrm[sl, :] = normed
        pt = dot(wt[u], normed, NT)
        mask = pm_ref[pl.ds(r, 1), :]
        left = mask * jax.nn.sigmoid(pt[ch:2 * ch]) * pt[:ch]
        right = mask * jax.nn.sigmoid(pt[3 * ch:]) * pt[2 * ch:3 * ch]
        if u == 0:
            fl[pl.ds(r, ch, stride=rows), :] = left
            fr[pl.ds(r, ch, stride=rows), :] = right
        elif hf == 0:
            fl[pl.ds(r, ch, stride=rows), :] = left
            fl[pl.ds(r + hr, ch, stride=rows), :] = right
        else:
            fr[pl.ds(r, ch, stride=rows), :] = left
            fr[pl.ds(r - hr, ch, stride=rows), :] = right

    def pack(k):
        pair = jnp.concatenate(
            [
                fl[k * block:(k + 1) * block, :].reshape(devs, rows, cols),
                fr[k * block:(k + 1) * block, :].reshape(devs, rows, cols),
            ],
            axis=1,
        )
        s_lr[k] = pair.astype(BF16)
        r_lr[k, c * nz + z] = s_lr[k, me]

    def send_first(k, near, far):
        ring(lambda zz, cc: s_lr.at[k, zz * nc + cc], r_lr.at[k, c * nz + z], sem_lr.at[0, k], sem_lr.at[1, k], near, far)

    def send_second(hf, k):
        src = fl if hf == 0 else fr
        s_l2[hf, k] = src[k * block:(k + 1) * block, :].reshape(devs, rows, cols).astype(BF16)
        r_l2[hf, k, c * nz + z] = s_l2[hf, k, me]
        scatter(
            lambda zz, cc: s_l2.at[hf, k, zz * nc + cc], r_l2.at[hf, k, c * nz + z],
            sem_l2.at[0, hf, k], sem_l2.at[1, hf, k])

    def gate_row(u, r):
        sl = pl.ds(pl.multiple_of(r * cols, cols), cols)
        gate[sl, :] = jax.nn.sigmoid(dot(nrm[sl, :], mp_ref[u, :, 4 * ch:], NN))

    def product(u, k):
        lefts, rights = [], []
        if u == 0:
            landed(r_lr.at[k], sem_lr.at[0, k], sem_lr.at[1, k]).wait_recv()
            for cc in range(nc):
                part = r_lr[k, cc * nz:(cc + 1) * nz].astype(F32)
                lefts.append(part[:, :rows].reshape(nz * rows, cols).astype(BF16))
                rights.append(part[:, rows:].reshape(nz * rows, cols).astype(BF16))
        else:
            for hf in range(2):
                landed(r_l2.at[hf, k], sem_l2.at[0, hf, k], sem_l2.at[1, hf, k]).wait_recv()
            low = lax.broadcasted_iota(jnp.int32, (nz, rows, cols), 1) < hr
            for cc in range(nc):
                first = r_l2[0, k, cc * nz:(cc + 1) * nz].astype(F32)
                last = r_l2[1, k, cc * nz:(cc + 1) * nz].astype(F32)
                lefts.append(jnp.where(low, first, last).reshape(nz * rows, cols).astype(BF16))
                turned = pltpu.roll(jnp.where(low, last, first), hr, 1)
                rights.append(turned.reshape(nz * rows, cols).astype(BF16))
        left = jnp.concatenate(lefts, axis=1)
        right = jnp.concatenate(rights, axis=1)
        prod = dot(left, right, NT if u == 0 else TN)
        tiles = [prod[:, cc * cols:(cc + 1) * cols].reshape(nz, rows, cols) for cc in range(nc)]
        if u or k == 0:
            n = u + k
            for cc in range(nc):
                s_p[n, cc] = tiles[cc].astype(BF16)
            r_p[n, me] = s_p[n, c, z]
            scatter(lambda zz, cc: s_p.at[n, cc, zz], r_p.at[n, me], sem_p.at[0, n], sem_p.at[1, n])
            return
        for hf in range(2):
            for cc in range(nc):
                s_q[hf, cc] = tiles[cc][:, hf * hr:(hf + 1) * hr].astype(BF16)
            r_q[hf, me] = s_q[hf, c, z]
            scatter(lambda zz, cc: s_q.at[hf, cc, zz], r_q.at[hf, me], sem_q.at[0, hf], sem_q.at[1, hf])

    def whole(n, k):
        landed(r_p.at[n], sem_p.at[0, n], sem_p.at[1, n]).wait_recv()
        fp[k * block:(k + 1) * block, :] = r_p[n].astype(F32).reshape(block, cols)

    def part(hf):
        landed(r_q.at[hf], sem_q.at[0, hf], sem_q.at[1, hf]).wait_recv()
        view = fp.reshape(ch, rows, cols)
        view[devs:, hf * hr:(hf + 1) * hr, :] = r_q[hf].astype(F32)

    def updated(u, r):
        sl = pl.ds(pl.multiple_of(r * cols, cols), cols)
        mixed = norm_sublanes(fp[pl.ds(r, ch, stride=rows), :], mgt[u]).astype(BF16)
        upd = dot(mixed, mo_ref[u], TN)
        src = x_ref if u == 0 else zb
        zb[sl, :] = (src[sl, :].astype(F32) + gate[sl, :] * upd).astype(BF16)

    def rows_loop(f, lo=0, hi=rows, step=2):
        def some(i, carry):
            for t in range(step):
                f(lo + i * step + t)
            return carry

        lax.fori_loop(0, (hi - lo) // step, some, 0)

    def first_row(r):
        project(0, r)

    rows_loop(first_row)
    pl.semaphore_wait(barrier, (2 * reach) * nc + 1)
    tell(reach, 0)
    pack(0)
    send_first(0, 1, reach)
    pack(1)
    send_first(1, 1, reach)
    for load in loads[4:]:
        load.wait()
    by_channel(1)
    hear(0)
    tell(2 * reach, 1)
    send_first(0, reach + 1, 2 * reach)
    send_first(1, reach + 1, 2 * reach)
    rows_loop(functools.partial(gate_row, 0))
    hear(1)
    send_first(0, 2 * reach + 1, half)
    send_first(1, 2 * reach + 1, half)
    for w in range(2):
        mgt[w] = jnp.transpose(jnp.broadcast_to(mg_ref[w:w + 1, :], (ch, ch)))
    for q in range(4):
        apt[q * ch:(q + 1) * ch, :] = jnp.transpose(
            ap_ref[:, q * ch:(q + 1) * ch].astype(F32)).astype(BF16)
    for k in range(per):
        product(0, k)
    whole(0, 0)
    for hf in range(2):
        part(hf)

        def both_steps(r, hf=hf):
            updated(0, r)
            project(1, r, hf)

        rows_loop(both_steps, hf * hr, (hf + 1) * hr)
        for k in range(per):
            send_second(hf, k)
    rows_loop(functools.partial(gate_row, 1))
    for k in range(per):
        product(1, k)

    def normed_row(r):
        sl = pl.ds(pl.multiple_of(r * cols, cols), cols)
        normed = norm_lanes(zb[sl, :].astype(F32), ag_ref[...]).astype(BF16)
        nall[c, sl, :] = normed
        fb[pl.ds(r, HEADS, stride=rows), :] = dot(ab_ref[...], normed, NT)

    whole(1, 0)
    whole(2, 1)

    def last_steps(r):
        updated(1, r)
        normed_row(r)

    rows_loop(last_steps, step=4)
    s_b[...] = fb[...].astype(BF16)
    to = z // half
    lots = half // stride
    many = nc * lots
    res = lax.rem(z, stride)
    turn = lax.rem(z, half) // stride
    slot = res * many + turn * nc + c
    hops = nz // stride

    def bias_wait(count, ssem, rsem):
        return remote(r_b.at[pl.ds(0, count)], r_b.at[pl.ds(0, count)], ssem, rsem, z, other)

    for t in sorted(range(1, hops), key=lambda t: -min(t, hops - t)):
        remote(s_b, r_b.at[slot], sem_b.at[0], sem_bf.at[turn], lax.rem(z + stride * t, nz), to).start()

    @pl.when(to == c)
    def _():
        r_b[slot] = s_b[...]

    @pl.when(to != c)
    def _():
        remote(s_b, r_b.at[slot], sem_b.at[0], sem_bf.at[turn], z, other).start()

    swap = remote(nall.at[c], nall.at[c], sem_n.at[0], sem_n.at[1], z, other)
    swap.start()

    def scores_row(r):
        sl = pl.ds(pl.multiple_of(r * cols, cols), cols)
        mine_n = nall[c, sl, :]
        full = jnp.concatenate([nall[cc, sl, :] for cc in range(nc)], axis=0)
        qt = dot(apt[:ch], mine_n, NT).astype(BF16)
        gt = dot(apt[3 * ch:], mine_n, NT).astype(BF16)
        keys = dot(full, ap_ref[:, ch:2 * ch], NN).astype(BF16)
        vt[r] = dot(apt[2 * ch:3 * ch], full, NT).astype(BF16)
        sg[r] = jax.nn.sigmoid(gt.astype(F32))
        wide = []
        for h in range(HEADS):
            parts = [jnp.zeros((h * hd, cols), BF16)] if h else []
            parts.append(qt[h * hd:(h + 1) * hd])
            if h < HEADS - 1:
                parts.append(jnp.zeros(((HEADS - 1 - h) * hd, cols), BF16))
            wide.append(jnp.concatenate(parts, axis=0))
        sc[r] = dot(keys, jnp.concatenate(wide, axis=1), NN) * (LOG2E / float(hd) ** 0.5)

    swap.wait()
    rows_loop(scores_row)

    for k in range(per):
        landed(r_lr.at[k], sem_lr.at[0, k], sem_lr.at[1, k]).wait_send()
        landed(r_q.at[k], sem_q.at[0, k], sem_q.at[1, k]).wait_send()
        for hf in range(2):
            landed(r_l2.at[hf, k], sem_l2.at[0, hf, k], sem_l2.at[1, hf, k]).wait_send()
    for n in range(3):
        landed(r_p.at[n], sem_p.at[0, n], sem_p.at[1, n]).wait_send()

    ahead = lax.rem(z + nz - c * half, nz)
    rising = (ahead < half // 2) | (ahead >= nz - half // 2)
    order = [jnp.where(rising, i, lots - 1 - i) for i in range(lots)]
    near = [lax.rem(z + nz + o, nz) for o in (2, 1, -1)]
    for m in order:
        here = c * half + m * stride + res == z

        @pl.when(here)
        def _(m=m):
            bias_wait(nc - 1, sem_b.at[0], sem_bf.at[m]).wait_recv()

        @pl.when(jnp.logical_not(here))
        def _(m=m):
            bias_wait(nc, sem_b.at[0], sem_bf.at[m]).wait_recv()

        group = r_b.at[pl.ds(res * many + m * nc, nc)]
        for beside in near:
            remote(group, group, sem_b.at[1], sem_bs.at[m], beside, c).start()

    for m in order:
        bias_wait(len(near) * nc, sem_b.at[1], sem_bs.at[m]).wait_recv()
    @pl.when(to == c)
    def _():
        bias_wait(hops - 1, sem_b.at[0], sem_bf.at[0]).wait_send()

    @pl.when(to != c)
    def _():
        bias_wait(hops, sem_b.at[0], sem_bf.at[0]).wait_send()

    bias_wait(len(near) * many, sem_b.at[1], sem_bf.at[0]).wait_send()
    for kc in range(nc):
        part = [
            jnp.stack([r_b[q * many + m * nc + kc] for m in range(lots)]).astype(F32) for q in range(stride)
        ]
        for h in range(HEADS):
            tile = jnp.stack([p[:, h * rows:(h + 1) * rows] for p in part], axis=1).reshape(half * rows, cols)
            tile = tile + km_ref[:, kc * cols:(kc + 1) * cols]
            bt[kc * cols:(kc + 1) * cols, h * cols:(h + 1) * cols] = jnp.transpose(tile * LOG2E)

    def attend_row(r):
        sl = pl.ds(pl.multiple_of(r * cols, cols), cols)
        score = sc[r] + bt[...]
        top = jnp.max(score, axis=0, keepdims=True)
        e = jnp.exp2(score - top)
        inv = 1.0 / jnp.sum(e, axis=0, keepdims=True)
        got = dot(vt[r], e.astype(BF16), NN)
        parts = []
        for h in range(HEADS):
            lanes = slice(h * cols, (h + 1) * cols)
            parts.append(got[h * hd:(h + 1) * hd, lanes] * inv[:, lanes])
        gated = (sg[r] * jnp.concatenate(parts, axis=0)).astype(BF16)
        ob[r] = (zb[sl, :].astype(F32) + dot(gated, ao_ref[...], TN)).astype(BF16)

    at_once = 4

    def leave(i):
        some = pl.ds(i * at_once, at_once)
        return pltpu.make_async_copy(ob.at[some], out_hbm.at[some], sem_o.at[i])

    def some_rows(i, carry):
        for t in range(at_once):
            attend_row(at_once * i + t)
        leave(i).start()
        return carry

    lax.fori_loop(0, rows // at_once, some_rows, 0)

    for i in range(rows // at_once):
        leave(i).wait()


def solution(mesh):
    nz, nc = mesh.shape["row"], mesh.shape["col"]
    devs = nz * nc

    def local(pair_rep, residue_mask, crop_length, norm_gain, mult_proj, mixed_gain, mult_out, att_gain, att_proj,
              att_bias, att_out):
        rows, cols, ch = pair_rep.shape
        per = ch // devs
        half = nz // 2
        stride = 4
        lots = half // stride
        area = rows * cols
        vmem = pltpu.VMEM
        out = pl.pallas_call(
            functools.partial(kernel, nz, nc, rows, stride, 4),
            out_shape=jax.ShapeDtypeStruct((rows, cols, ch), BF16),
            in_specs=[pl.BlockSpec(memory_space=pltpu.SMEM)] + [pl.BlockSpec(memory_space=pl.ANY)] * 10,
            out_specs=pl.BlockSpec(memory_space=pl.ANY),
            scratch_shapes=[
                vmem((1, nc * cols), jnp.int32),
                vmem((area, ch), BF16),
                vmem(norm_gain.shape, F32),
                vmem(mult_proj.shape, BF16),
                vmem(mixed_gain.shape, F32),
                vmem(mult_out.shape, BF16),
                vmem((1, ch), F32),
                vmem(att_proj.shape, BF16),
                vmem((HEADS, ch), BF16),
                vmem(att_out.shape, BF16),
                pltpu.SemaphoreType.DMA((10,)),
                vmem((rows, cols), F32),
                vmem((1, nc * cols), F32),
                vmem((2, 4 * ch, ch), BF16),
                vmem((2, ch, ch), F32),
                vmem((4 * ch, ch), BF16),
                vmem((area, ch), BF16),
                vmem((area, ch), F32),
                vmem((area, ch), BF16),
                vmem((ch * rows, cols), F32),
                vmem((ch * rows, cols), F32),
                vmem((ch * rows, cols), F32),
                vmem((per, devs, 2 * rows, cols), BF16),
                vmem((per, devs, 2 * rows, cols), BF16),
                vmem((2, per, devs, rows, cols), BF16),
                vmem((2, per, devs, rows, cols), BF16),
                vmem((3, nc, nz, rows, cols), BF16),
                vmem((3, devs, rows, cols), BF16),
                vmem((2, nc, nz, rows // 2, cols), BF16),
                vmem((2, devs, rows // 2, cols), BF16),
                vmem((nc, area, ch), BF16),
                vmem((HEADS * rows, cols), F32),
                vmem((HEADS * rows, cols), BF16),
                vmem((nc * half, HEADS * rows, cols), BF16),
                vmem((nc * cols, HEADS * cols), F32),
                vmem((rows, nc * cols, HEADS * cols), F32),
                vmem((rows, ch, nc * cols), BF16),
                vmem((rows, ch, cols), F32),
                vmem((rows, cols, ch), BF16),
                pltpu.SemaphoreType.REGULAR((2, 2)),
                pltpu.SemaphoreType.DMA((2, per)),
                pltpu.SemaphoreType.DMA((2, 2, per)),
                pltpu.SemaphoreType.DMA((2, 3)),
                pltpu.SemaphoreType.DMA((2, 2)),
                pltpu.SemaphoreType.DMA((2,)),
                pltpu.SemaphoreType.DMA((lots,)),
                pltpu.SemaphoreType.DMA((lots,)),
                pltpu.SemaphoreType.DMA((2,)),
                pltpu.SemaphoreType.DMA((rows // 2,)),
            ],
            compiler_params=pltpu.CompilerParams(
                collective_id=1, has_side_effects=True, vmem_limit_bytes=62 * 1024 * 1024
            ),
            name="triangle",
        )(
            crop_length, residue_mask.reshape(1, nc * cols), pair_rep.reshape(area, ch), norm_gain, mult_proj,
            mixed_gain, mult_out, att_gain.reshape(1, ch), att_proj, att_bias.T, att_out,
        )
        return out

    return jax.shard_map(
        local,
        mesh=mesh,
        in_specs=(P(("groups", "row"), "col", None), P("groups"), P("groups")) + (P(),) * 8,
        out_specs=P(("groups", "row"), "col", None),
        check_vma=False,
    )
```

```python
import functools

import jax
import jax.numpy as jnp
from jax import lax
from jax.experimental import pallas as pl
from jax.experimental.pallas import tpu as pltpu
from jax.sharding import PartitionSpec as P

HEADS = 4
EPSILON = 1e-05
LOG2E = 1.4426950408889634
MESH = pl.DeviceIdType.MESH
F32 = jnp.float32
BF16 = jnp.bfloat16
NN = (((1,), (0,)), ((), ()))
NT = (((1,), (1,)), ((), ()))
TN = (((0,), (0,)), ((), ()))


def dot(a, b, dims):
    return lax.dot_general(a, b, dims, preferred_element_type=F32)


def norm_lanes(v, gain):
    mean = jnp.mean(v, axis=-1, keepdims=True)
    cen = v - mean
    var = jnp.mean(cen * cen, axis=-1, keepdims=True)
    return cen * lax.rsqrt(var + EPSILON) * gain


def norm_sublanes(v, gain):
    mean = jnp.mean(v, axis=0, keepdims=True)
    cen = v - mean
    var = jnp.mean(cen * cen, axis=0, keepdims=True)
    return cen * lax.rsqrt(var + EPSILON) * gain


def kernel(
    nz, nc, rows, stride, reach, crop_ref, rm_hbm, x_hbm, ng_hbm, mp_hbm, mg_hbm, mo_hbm, ag_hbm, ap_hbm, ab_hbm, ao_hbm,
    out_hbm,
    rm_ref, x_ref, ng_ref, mp_ref, mg_ref, mo_ref, ag_ref, ap_ref, ab_ref, ao_ref, sem_in,
    pm_ref, km_ref, wt, mgt, apt, nrm, gate, zb, fl, fr, fp, s_lr, r_lr, s_l2, r_l2, s_p, r_p, s_q, r_q, nall, fb, s_b, r_b, bt, sc, vt, sg, ob,
    level, sem_lr, sem_l2, sem_p, sem_q, sem_n, sem_bf, sem_bs, sem_b, sem_o,
):
    z = lax.axis_index("row")
    c = lax.axis_index("col")
    me = z * nc + c
    devs = nz * nc
    cols = pm_ref.shape[1]
    ch = x_ref.shape[1]
    hd = ch // HEADS
    per = s_lr.shape[0]
    block = devs * rows
    half = nz // 2
    other = 1 - c

    barrier = pltpu.get_barrier_semaphore()

    for d in range(1, reach + 1):
        for zz in (lax.rem(z + d, nz), lax.rem(z + nz - d, nz)):
            for cc in (c, other):
                pl.semaphore_signal(barrier, inc=1, device_id={"row": zz, "col": cc}, device_id_type=MESH)
    pl.semaphore_signal(barrier, inc=1, device_id={"row": z, "col": other}, device_id_type=MESH)
    loads = []
    for i, (src, dst) in enumerate((
        (x_hbm, x_ref), (ng_hbm, ng_ref), (mp_hbm, mp_ref), (rm_hbm, rm_ref), (mg_hbm, mg_ref), (mo_hbm, mo_ref),
        (ag_hbm, ag_ref), (ap_hbm, ap_ref), (ab_hbm, ab_ref), (ao_hbm, ao_ref),
    )):
        loads.append(pltpu.make_async_copy(src, dst, sem_in.at[i]))
        loads[-1].start()

    def tell(d, n):
        up, down = lax.rem(z + d, nz), lax.rem(z + nz - d, nz)
        pl.semaphore_signal(level.at[0, n], inc=1, device_id={"row": up, "col": c}, device_id_type=MESH)
        pl.semaphore_signal(level.at[1, n], inc=1, device_id={"row": down, "col": c}, device_id_type=MESH)

    def hear(n):
        pl.semaphore_wait(level.at[0, n], 1)
        pl.semaphore_wait(level.at[1, n], 1)

    def remote(src, dst, ssem, rsem, zz, cc):
        return pltpu.make_async_remote_copy(
            src_ref=src, dst_ref=dst, send_sem=ssem, recv_sem=rsem,
            device_id={"row": zz, "col": cc}, device_id_type=MESH,
        )

    def ring(src_at, dst, ssem, rsem, near, far):
        def put(zz):
            remote(src_at(zz, c), dst, ssem, rsem, zz, c).start()
            remote(src_at(zz, other), dst, ssem, rsem, zz, other).start()

        def both(i, carry):
            up, down = z + far - i, z - far + i
            put(jnp.where(up >= nz, up - nz, up))
            put(jnp.where(down < 0, down + nz, down))
            return carry

        if far == half:
            put(lax.rem(z + half, nz))
            far -= 1
        lax.fori_loop(0, far + 1 - near, both, 0)
        if near == 1:
            remote(src_at(z, other), dst, ssem, rsem, z, other).start()

    def scatter(src_at, dst, ssem, rsem):
        ring(src_at, dst, ssem, rsem, 1, half)

    def landed(buf, ssem, rsem):
        every = buf.at[pl.ds(0, devs - 1)]
        return remote(every, every, ssem, rsem, z, other)

    for load in loads[:4]:
        load.wait()
    pos = lax.broadcasted_iota(jnp.int32, rm_ref.shape, 1)
    alive = jnp.where(((rm_ref[...] == 1) | (pos == 0)) & (pos < crop_ref[0]), 1.0, 0.0).astype(F32)
    km_ref[...] = jnp.where(alive > 0.0, 0.0, -1000000000.0).astype(F32)
    spot = lax.broadcasted_iota(jnp.int32, (rows, nc * cols), 1)
    want = lax.broadcasted_iota(jnp.int32, (rows, nc * cols), 0) + z * rows
    row_alive = jnp.sum(jnp.where(spot == want, alive, 0.0), axis=1, keepdims=True)
    col_alive = alive[:, :cols]
    for cc in range(1, nc):
        col_alive = jnp.where(c == cc, alive[:, cc * cols:(cc + 1) * cols], col_alive)
    pm_ref[:rows, :] = row_alive * col_alive

    def by_channel(u):
        for q in range(4):
            wt[u, q * ch:(q + 1) * ch, :] = jnp.transpose(
                mp_ref[u, :, q * ch:(q + 1) * ch].astype(F32)).astype(BF16)

    by_channel(0)

    hr = rows // 2

    def project(u, r, hf=0):
        sl = pl.ds(pl.multiple_of(r * cols, cols), cols)
        src = x_ref if u == 0 else zb
        normed = norm_lanes(src[sl, :].astype(F32), ng_ref[u:u + 1, :]).astype(BF16)
        nrm[sl, :] = normed
        pt = dot(wt[u], normed, NT)
        mask = pm_ref[pl.ds(r, 1), :]
        left = mask * jax.nn.sigmoid(pt[ch:2 * ch]) * pt[:ch]
        right = mask * jax.nn.sigmoid(pt[3 * ch:]) * pt[2 * ch:3 * ch]
        if u == 0:
            fl[pl.ds(r, ch, stride=rows), :] = left
            fr[pl.ds(r, ch, stride=rows), :] = right
        elif hf == 0:
            fl[pl.ds(r, ch, stride=rows), :] = left
            fl[pl.ds(r + hr, ch, stride=rows), :] = right
        else:
            fr[pl.ds(r, ch, stride=rows), :] = left
            fr[pl.ds(r - hr, ch, stride=rows), :] = right

    def pack(k):
        pair = jnp.concatenate(
            [
                fl[k * block:(k + 1) * block, :].reshape(devs, rows, cols),
                fr[k * block:(k + 1) * block, :].reshape(devs, rows, cols),
            ],
            axis=1,
        )
        s_lr[k] = pair.astype(BF16)
        r_lr[k, c * nz + z] = s_lr[k, me]

    def send_first(k, near, far):
        ring(lambda zz, cc: s_lr.at[k, zz * nc + cc], r_lr.at[k, c * nz + z], sem_lr.at[0, k], sem_lr.at[1, k], near, far)

    def send_second(hf, k):
        src = fl if hf == 0 else fr
        s_l2[hf, k] = src[k * block:(k + 1) * block, :].reshape(devs, rows, cols).astype(BF16)
        r_l2[hf, k, c * nz + z] = s_l2[hf, k, me]
        scatter(
            lambda zz, cc: s_l2.at[hf, k, zz * nc + cc], r_l2.at[hf, k, c * nz + z],
            sem_l2.at[0, hf, k], sem_l2.at[1, hf, k])

    def gate_row(u, r):
        sl = pl.ds(pl.multiple_of(r * cols, cols), cols)
        gate[sl, :] = jax.nn.sigmoid(dot(nrm[sl, :], mp_ref[u, :, 4 * ch:], NN))

    def product(u, k):
        lefts, rights = [], []
        if u == 0:
            landed(r_lr.at[k], sem_lr.at[0, k], sem_lr.at[1, k]).wait_recv()
            for cc in range(nc):
                part = r_lr[k, cc * nz:(cc + 1) * nz].astype(F32)
                lefts.append(part[:, :rows].reshape(nz * rows, cols).astype(BF16))
                rights.append(part[:, rows:].reshape(nz * rows, cols).astype(BF16))
        else:
            for hf in range(2):
                landed(r_l2.at[hf, k], sem_l2.at[0, hf, k], sem_l2.at[1, hf, k]).wait_recv()
            low = lax.broadcasted_iota(jnp.int32, (nz, rows, cols), 1) < hr
            for cc in range(nc):
                first = r_l2[0, k, cc * nz:(cc + 1) * nz].astype(F32)
                last = r_l2[1, k, cc * nz:(cc + 1) * nz].astype(F32)
                lefts.append(jnp.where(low, first, last).reshape(nz * rows, cols).astype(BF16))
                turned = pltpu.roll(jnp.where(low, last, first), hr, 1)
                rights.append(turned.reshape(nz * rows, cols).astype(BF16))
        left = jnp.concatenate(lefts, axis=1)
        right = jnp.concatenate(rights, axis=1)
        prod = dot(left, right, NT if u == 0 else TN)
        tiles = [prod[:, cc * cols:(cc + 1) * cols].reshape(nz, rows, cols) for cc in range(nc)]
        if u or k == 0:
            n = u + k
            for cc in range(nc):
                s_p[n, cc] = tiles[cc].astype(BF16)
            r_p[n, me] = s_p[n, c, z]
            scatter(lambda zz, cc: s_p.at[n, cc, zz], r_p.at[n, me], sem_p.at[0, n], sem_p.at[1, n])
            return
        for hf in range(2):
            for cc in range(nc):
                s_q[hf, cc] = tiles[cc][:, hf * hr:(hf + 1) * hr].astype(BF16)
            r_q[hf, me] = s_q[hf, c, z]
            scatter(lambda zz, cc: s_q.at[hf, cc, zz], r_q.at[hf, me], sem_q.at[0, hf], sem_q.at[1, hf])

    def whole(n, k):
        landed(r_p.at[n], sem_p.at[0, n], sem_p.at[1, n]).wait_recv()
        fp[k * block:(k + 1) * block, :] = r_p[n].astype(F32).reshape(block, cols)

    def part(hf):
        landed(r_q.at[hf], sem_q.at[0, hf], sem_q.at[1, hf]).wait_recv()
        view = fp.reshape(ch, rows, cols)
        view[devs:, hf * hr:(hf + 1) * hr, :] = r_q[hf].astype(F32)

    def updated(u, r):
        sl = pl.ds(pl.multiple_of(r * cols, cols), cols)
        mixed = norm_sublanes(fp[pl.ds(r, ch, stride=rows), :], mgt[u]).astype(BF16)
        upd = dot(mixed, mo_ref[u], TN)
        src = x_ref if u == 0 else zb
        zb[sl, :] = (src[sl, :].astype(F32) + gate[sl, :] * upd).astype(BF16)

    def rows_loop(f, lo=0, hi=rows, step=2):
        def some(i, carry):
            for t in range(step):
                f(lo + i * step + t)
            return carry

        lax.fori_loop(0, (hi - lo) // step, some, 0)

    def first_row(r):
        project(0, r)

    rows_loop(first_row)
    pl.semaphore_wait(barrier, (2 * reach) * nc + 1)
    tell(reach, 0)
    pack(0)
    send_first(0, 1, reach)
    pack(1)
    send_first(1, 1, reach)
    for load in loads[4:]:
        load.wait()
    by_channel(1)
    hear(0)
    tell(2 * reach, 1)
    send_first(0, reach + 1, 2 * reach)
    send_first(1, reach + 1, 2 * reach)
    rows_loop(functools.partial(gate_row, 0))
    hear(1)
    send_first(0, 2 * reach + 1, half)
    send_first(1, 2 * reach + 1, half)
    for w in range(2):
        mgt[w] = jnp.transpose(jnp.broadcast_to(mg_ref[w:w + 1, :], (ch, ch)))
    for q in range(4):
        apt[q * ch:(q + 1) * ch, :] = jnp.transpose(
            ap_ref[:, q * ch:(q + 1) * ch].astype(F32)).astype(BF16)
    for k in range(per):
        product(0, k)
    whole(0, 0)
    for hf in range(2):
        part(hf)

        def both_steps(r, hf=hf):
            updated(0, r)
            project(1, r, hf)

        rows_loop(both_steps, hf * hr, (hf + 1) * hr)
        for k in range(per):
            send_second(hf, k)
    rows_loop(functools.partial(gate_row, 1))
    for k in range(per):
        product(1, k)

    def normed_row(r):
        sl = pl.ds(pl.multiple_of(r * cols, cols), cols)
        normed = norm_lanes(zb[sl, :].astype(F32), ag_ref[...]).astype(BF16)
        nall[c, sl, :] = normed
        fb[pl.ds(r, HEADS, stride=rows), :] = dot(ab_ref[...], normed, NT)

    whole(1, 0)
    whole(2, 1)

    def last_steps(r):
        updated(1, r)
        normed_row(r)

    rows_loop(last_steps, step=4)
    s_b[...] = fb[:HEADS * rows, :].astype(BF16)
    to = z // half
    lots = half // stride
    many = nc * lots
    res = lax.rem(z, stride)
    turn = lax.rem(z, half) // stride
    slot = res * many + turn * nc + c
    hops = nz // stride

    def bias_wait(count, ssem, rsem):
        return remote(r_b.at[pl.ds(0, count)], r_b.at[pl.ds(0, count)], ssem, rsem, z, other)

    for t in sorted(range(1, hops), key=lambda t: -min(t, hops - t)):
        remote(s_b, r_b.at[slot], sem_b.at[0], sem_bf.at[turn], lax.rem(z + stride * t, nz), to).start()

    @pl.when(to == c)
    def _():
        r_b[slot] = s_b[...]

    @pl.when(to != c)
    def _():
        remote(s_b, r_b.at[slot], sem_b.at[0], sem_bf.at[turn], z, other).start()

    swap = remote(nall.at[c], nall.at[c], sem_n.at[0], sem_n.at[1], z, other)
    swap.start()

    def scores_row(r):
        sl = pl.ds(pl.multiple_of(r * cols, cols), cols)
        mine_n = nall[c, sl, :]
        full = jnp.concatenate([nall[cc, sl, :] for cc in range(nc)], axis=0)
        qt = dot(apt[:ch], mine_n, NT).astype(BF16)
        gt = dot(apt[3 * ch:], mine_n, NT).astype(BF16)
        keys = dot(full, ap_ref[:, ch:2 * ch], NN).astype(BF16)
        vt[r] = dot(apt[2 * ch:3 * ch], full, NT).astype(BF16)
        sg[r] = jax.nn.sigmoid(gt.astype(F32))
        wide = []
        for h in range(HEADS):
            parts = [jnp.zeros((h * hd, cols), BF16)] if h else []
            parts.append(qt[h * hd:(h + 1) * hd])
            if h < HEADS - 1:
                parts.append(jnp.zeros(((HEADS - 1 - h) * hd, cols), BF16))
            wide.append(jnp.concatenate(parts, axis=0))
        sc[r] = dot(keys, jnp.concatenate(wide, axis=1), NN) * (LOG2E / float(hd) ** 0.5)

    swap.wait()
    rows_loop(scores_row)

    for k in range(per):
        landed(r_lr.at[k], sem_lr.at[0, k], sem_lr.at[1, k]).wait_send()
        landed(r_q.at[k], sem_q.at[0, k], sem_q.at[1, k]).wait_send()
        for hf in range(2):
            landed(r_l2.at[hf, k], sem_l2.at[0, hf, k], sem_l2.at[1, hf, k]).wait_send()
    for n in range(3):
        landed(r_p.at[n], sem_p.at[0, n], sem_p.at[1, n]).wait_send()

    ahead = lax.rem(z + nz - c * half, nz)
    rising = (ahead < half // 2) | (ahead >= nz - half // 2)
    order = [jnp.where(rising, i, lots - 1 - i) for i in range(lots)]
    near = [lax.rem(z + nz + o, nz) for o in (2, 1, -1)]
    for m in order:
        here = c * half + m * stride + res == z

        @pl.when(here)
        def _(m=m):
            bias_wait(nc - 1, sem_b.at[0], sem_bf.at[m]).wait_recv()

        @pl.when(jnp.logical_not(here))
        def _(m=m):
            bias_wait(nc, sem_b.at[0], sem_bf.at[m]).wait_recv()

        group = r_b.at[pl.ds(res * many + m * nc, nc)]
        for beside in near:
            remote(group, group, sem_b.at[1], sem_bs.at[m], beside, c).start()

    for m in order:
        bias_wait(len(near) * nc, sem_b.at[1], sem_bs.at[m]).wait_recv()
    @pl.when(to == c)
    def _():
        bias_wait(hops - 1, sem_b.at[0], sem_bf.at[0]).wait_send()

    @pl.when(to != c)
    def _():
        bias_wait(hops, sem_b.at[0], sem_bf.at[0]).wait_send()

    bias_wait(len(near) * many, sem_b.at[1], sem_bf.at[0]).wait_send()
    for kc in range(nc):
        part = [
            jnp.stack([r_b[q * many + m * nc + kc] for m in range(lots)]).astype(F32) for q in range(stride)
        ]
        for h in range(HEADS):
            tile = jnp.stack([p[:, h * rows:(h + 1) * rows] for p in part], axis=1).reshape(half * rows, cols)
            tile = tile + km_ref[:, kc * cols:(kc + 1) * cols]
            bt[kc * cols:(kc + 1) * cols, h * cols:(h + 1) * cols] = jnp.transpose(tile * LOG2E)

    def attend_row(r):
        sl = pl.ds(pl.multiple_of(r * cols, cols), cols)
        score = sc[r] + bt[...]
        top = jnp.max(score, axis=0, keepdims=True)
        e = jnp.exp2(score - top)
        inv = 1.0 / jnp.sum(e, axis=0, keepdims=True)
        got = dot(vt[r], e.astype(BF16), NN)
        parts = []
        for h in range(HEADS):
            lanes = slice(h * cols, (h + 1) * cols)
            parts.append(got[h * hd:(h + 1) * hd, lanes] * inv[:, lanes])
        gated = (sg[r] * jnp.concatenate(parts, axis=0)).astype(BF16)
        ob[r] = (zb[sl, :].astype(F32) + dot(gated, ao_ref[...], TN)).astype(BF16)

    at_once = 4

    def leave(i):
        some = pl.ds(i * at_once, at_once)
        return pltpu.make_async_copy(ob.at[some], out_hbm.at[some], sem_o.at[i])

    def some_rows(i, carry):
        for t in range(at_once):
            attend_row(at_once * i + t)
        leave(i).start()
        return carry

    lax.fori_loop(0, rows // at_once, some_rows, 0)

    for i in range(rows // at_once):
        leave(i).wait()


def solution(mesh):
    nz, nc = mesh.shape["row"], mesh.shape["col"]
    devs = nz * nc

    def local(pair_rep, residue_mask, crop_length, norm_gain, mult_proj, mixed_gain, mult_out, att_gain, att_proj,
              att_bias, att_out):
        rows, cols, ch = pair_rep.shape
        per = ch // devs
        half = nz // 2
        stride = 4
        lots = half // stride
        area = rows * cols
        vmem = pltpu.VMEM
        out = pl.pallas_call(
            functools.partial(kernel, nz, nc, rows, stride, 4),
            out_shape=jax.ShapeDtypeStruct((rows, cols, ch), BF16),
            in_specs=[pl.BlockSpec(memory_space=pltpu.SMEM)] + [pl.BlockSpec(memory_space=pl.ANY)] * 10,
            out_specs=pl.BlockSpec(memory_space=pl.ANY),
            scratch_shapes=[
                vmem((1, nc * cols), jnp.int32),
                vmem((area, ch), BF16),
                vmem(norm_gain.shape, F32),
                vmem(mult_proj.shape, BF16),
                vmem(mixed_gain.shape, F32),
                vmem(mult_out.shape, BF16),
                vmem((1, ch), F32),
                vmem(att_proj.shape, BF16),
                vmem((HEADS, ch), BF16),
                vmem(att_out.shape, BF16),
                pltpu.SemaphoreType.DMA((10,)),
                vmem((2 * rows, cols), F32),
                vmem((1, nc * cols), F32),
                vmem((2, 4 * ch, ch), BF16),
                vmem((2, ch, ch), F32),
                vmem((4 * ch, ch), BF16),
                vmem((area, ch), BF16),
                vmem((area, ch), F32),
                vmem((area, ch), BF16),
                vmem((ch * rows, cols), F32),
                vmem((ch * rows, cols), F32),
                vmem((ch * rows, cols), F32),
                vmem((per, devs, 2 * rows, cols), BF16),
                vmem((per, devs, 2 * rows, cols), BF16),
                vmem((2, per, devs, rows, cols), BF16),
                vmem((2, per, devs, rows, cols), BF16),
                vmem((3, nc, nz, rows, cols), BF16),
                vmem((3, devs, rows, cols), BF16),
                vmem((2, nc, nz, rows // 2, cols), BF16),
                vmem((2, devs, rows // 2, cols), BF16),
                vmem((nc, area, ch), BF16),
                vmem((8 * rows, cols), F32),
                vmem((HEADS * rows, cols), BF16),
                vmem((nc * half, HEADS * rows, cols), BF16),
                vmem((nc * cols, HEADS * cols), F32),
                vmem((rows, nc * cols, HEADS * cols), F32),
                vmem((rows, ch, nc * cols), BF16),
                vmem((rows, ch, cols), F32),
                vmem((rows, cols, ch), BF16),
                pltpu.SemaphoreType.REGULAR((2, 2)),
                pltpu.SemaphoreType.DMA((2, per)),
                pltpu.SemaphoreType.DMA((2, 2, per)),
                pltpu.SemaphoreType.DMA((2, 3)),
                pltpu.SemaphoreType.DMA((2, 2)),
                pltpu.SemaphoreType.DMA((2,)),
                pltpu.SemaphoreType.DMA((lots,)),
                pltpu.SemaphoreType.DMA((lots,)),
                pltpu.SemaphoreType.DMA((2,)),
                pltpu.SemaphoreType.DMA((rows // 2,)),
            ],
            compiler_params=pltpu.CompilerParams(
                collective_id=1, has_side_effects=True, vmem_limit_bytes=62 * 1024 * 1024
            ),
            name="triangle",
        )(
            crop_length, residue_mask.reshape(1, nc * cols), pair_rep.reshape(area, ch), norm_gain, mult_proj,
            mixed_gain, mult_out, att_gain.reshape(1, ch), att_proj, att_bias.T, att_out,
        )
        return out

    return jax.shard_map(
        local,
        mesh=mesh,
        in_specs=(P(("groups", "row"), "col", None), P("groups"), P("groups")) + (P(),) * 8,
        out_specs=P(("groups", "row"), "col", None),
        check_vma=False,
    )
```
